128 devices in a mesh: gx: 16 (over x, y), gy: 8 (over z, core).
Axes of the slice: x: 4, y: 4, z: 4, core: 2. Of those that a mesh axis runs over, the one named last changes fastest.
Arguments:
- sat_new: float32 [64, 1024, 1024], P(None, 'gx', 'gy'), may hold values from 0.02 to 1
- sat_old: float32 [64, 1024, 1024], P(None, 'gx', 'gy'), may hold values from 0.1 to 0.95
- porosity: float32 [64, 1024, 1024], P(None, 'gx', 'gy'), may hold values from 0.1 to 0.5
- spec_storage: float32 [64, 1024, 1024], P(None, 'gx', 'gy'), may hold values from 0.01 to 0.2
- pressure: float32 [64, 1024, 1024], P(None, 'gx', 'gy'), may hold values from -6 to 6
- conduct: float32 [64, 1024, 1024], P(None, 'gx', 'gy'), may hold values from 0.1 to 1
- et_rate: float32 [64, 1024, 1024], P(None, 'gx', 'gy'), may hold values from 0 to 1
- thickness: float32 [64], replicated, may hold values from 0.005 to 0.05
- labels: int32 [1024, 1024], P('gx', 'gy'), may hold values from 0 to 511, as said below
- outlet: int32 [1024, 1024], P('gx', 'gy'), may hold values 0 or 1
Outputs:
- basin_totals: float32 [4, 64, 512], replicated
- column_balance: float32 [4, 1024, 1024], P(None, 'gx', 'gy')
- peak_change: float32 [], replicated
The draws below stay inside these ranges and needn't reach their ends.
Inputs may be any that keep to these rules, and one draw needn't show every extreme that they name: `labels`: subbasins are contiguous patches of columns with ragged edges.
All inputs are finite; a program needn't handle non-finite values. No bound on the sum of `outlet` on one device may be relied on, other than what follows from the above.
Results may differ from the reference program's by a relative error of at most 0.00016.
Values sent between devices are 32-bit elements; how exact they have to be, the bound alone decides.
A program may use at most 128 MiB of HBM per device.

```python
import math
import jax
import jax.numpy as jnp

NZ = 64
SUB = 512
CX = 64
CY = 128
NX = 1024
NY = 1024


def saturation_pair(key):
    first, second, third = jax.random.split(jax.random.fold_in(key, 7301), 3)
    older = jax.random.uniform(first, (NZ, NX, NY), jnp.float32, 0.2, 0.9)
    noise = jax.random.normal(second, (NZ, NX, NY), jnp.float32)
    blocks_x = NX // CX
    blocks_y = NY // CY
    amp_log = jax.random.uniform(third, (blocks_x, blocks_y), jnp.float32, jnp.log(0.01), jnp.log(0.3))
    amp = jnp.exp(amp_log)
    amp_full = jnp.repeat(jnp.repeat(amp, CX, axis=0), CY, axis=1)
    newer = jnp.clip(older + noise * amp_full[None], 0.02, 1.0)
    return (older, newer)


def draw_sat_new(key, part):
    older, newer = saturation_pair(key)
    return newer


def draw_sat_old(key, part):
    older, newer = saturation_pair(key)
    return older


def draw_labels(key, part):
    first, second, third = jax.random.split(jax.random.fold_in(key, 911), 3)
    rows_x = jnp.arange(NX, dtype=jnp.int32)[:, None]
    rows_y = jnp.arange(NY, dtype=jnp.int32)[None, :]
    jitter_x = jax.random.randint(first, (NX, NY), -4, 5, dtype=jnp.int32)
    jitter_y = jax.random.randint(second, (NX, NY), -4, 5, dtype=jnp.int32)
    moved_x = jnp.clip(rows_x + jitter_x, 0, NX - 1)
    moved_y = jnp.clip(rows_y + jitter_y, 0, NY - 1)
    across = SUB // 32
    region = moved_x * 32 // NX * across + moved_y * across // NY
    order = jax.random.permutation(third, SUB).astype(jnp.int32)
    return order[region].astype(jnp.int32)


def with_ends(drawn, own_key, smallest, top_value):
    longest = drawn.shape.index(max(drawn.shape))
    spots = []
    for shift in (0, 1):
        where = [jax.random.randint(jax.random.fold_in(own_key, axis), (), 0, length) for axis, length in enumerate(drawn.shape)]
        where[longest] = (where[longest] + shift) % drawn.shape[longest]
        spots.append(tuple(where))
    return drawn.at[spots[0]].set(smallest).at[spots[1]].set(top_value)


def block_scale(stream_key, shape, shards, least, top_value):
    def one(position, shards_of):
        steps = jax.random.uniform(jax.random.fold_in(jax.random.fold_in(stream_key, 6), position), (shards_of,), jnp.float32, least / len(shards), top_value / len(shards))
        return jnp.repeat(jnp.exp(steps), shape[position] // shards_of).reshape((-1,) + (1,) * (len(shape) - position - 1))

    level = one(*shards[0])
    for cut in shards[1:]:
        level = level * one(*cut)
    return level


def scatter_about(key, extent, deviation, most, cuts=(), kind=jnp.bfloat16):
    gain = block_scale(key, extent, cuts, -0.22, 0.18) if cuts else 1.0
    result = jax.random.normal(key, extent, jnp.float32) * deviation * gain
    return jnp.minimum(jnp.maximum(result, -most), most).astype(kind)


def setup_inputs(seed: int = 0) -> dict:
    streams_of = jax.random.split(jax.random.key(seed), 11)
    sat_new = draw_sat_new(jax.random.fold_in(streams_of[10], 71), 0)
    sat_old = draw_sat_old(jax.random.fold_in(streams_of[10], 71), 0)
    porosity = jnp.clip(0.1 + 0.4 * jax.random.uniform(streams_of[2], (NZ, NX, NY), jnp.float32) ** block_scale(streams_of[2], (NZ, NX, NY), ((1, 16), (2, 8)), -0.2, 0.2), 0.1, 0.5)
    spec_storage = jnp.clip(jnp.exp(math.log(0.2) - 2.9957323 * jax.random.uniform(streams_of[3], (NZ, NX, NY), jnp.float32) ** block_scale(streams_of[3], (NZ, NX, NY), ((1, 16), (2, 8)), -0.2, 0.2)), 0.01, 0.2)
    pressure = scatter_about(streams_of[4], (NZ, NX, NY), 1.0, 6.0, ((1, 16), (2, 8)), jnp.float32)
    conduct = jnp.clip(jnp.exp(math.log(1.0) - 2.3025851 * jax.random.uniform(streams_of[5], (NZ, NX, NY), jnp.float32) ** block_scale(streams_of[5], (NZ, NX, NY), ((1, 16), (2, 8)), -0.2, 0.2)), 0.1, 1.0)
    et_rate = jnp.clip(1.0 * jax.random.uniform(streams_of[6], (NZ, NX, NY), jnp.float32) ** block_scale(streams_of[6], (NZ, NX, NY), ((1, 16), (2, 8)), -0.2, 0.2), 0.0, 1.0)
    thickness = jnp.clip(jnp.exp(jax.random.uniform(streams_of[7], (NZ,), jnp.float32, math.log(0.005), math.log(0.05))), 0.005, 0.05)
    labels = draw_labels(jax.random.fold_in(streams_of[10], 71), 0)
    outlet = with_ends((jax.random.randint(streams_of[9], (NX, NY), 0, 8) < 1).astype(jnp.int32), jax.random.fold_in(streams_of[9], 1), 0, 1)
    return dict(sat_new=sat_new, sat_old=sat_old, porosity=porosity, spec_storage=spec_storage, pressure=pressure, conduct=conduct, et_rate=et_rate, thickness=thickness, labels=labels, outlet=outlet)


def lateral_flux(pressure, conduct, depth):
    padded_p = jnp.pad(pressure, ((0, 0), (1, 1), (1, 1)))
    padded_k = jnp.pad(conduct, ((0, 0), (1, 1), (1, 1)))
    cx = pressure.shape[1]
    cy = pressure.shape[2]
    total = jnp.zeros(pressure.shape, jnp.float32)
    for shift_i, shift_j in ((0, 1), (2, 1), (1, 0), (1, 2)):
        near_p = padded_p[:, shift_i:shift_i + cx, shift_j:shift_j + cy]
        near_k = padded_k[:, shift_i:shift_i + cx, shift_j:shift_j + cy]
        face = 2.0 * conduct * near_k / (conduct + near_k)
        total = total + face * (pressure - near_p)
    return depth * total


def reference(sat_new, sat_old, porosity, spec_storage, pressure, conduct, et_rate, thickness, labels, outlet):
    depth = thickness[:, None, None]
    flux = lateral_flux(pressure, conduct, depth)
    water = depth * sat_new * (porosity + spec_storage * pressure)
    change = depth * porosity * (sat_new - sat_old)
    uptake = depth * et_rate
    fields = jnp.stack([water, change, uptake, flux])
    column_balance = jnp.sum(fields, axis=1)
    masked = jnp.concatenate([fields[:3], fields[3:] * outlet.astype(jnp.float32)[None, None]], axis=0)
    rows = masked.reshape(4 * NZ, NX * NY)
    flat_labels = labels.reshape(-1).astype(jnp.int32)
    summed = jax.ops.segment_sum(rows.T, flat_labels, num_segments=SUB)
    basin_scale = NZ * SUB / (NX * NY)
    basin_totals = (summed.T.reshape(4, NZ, SUB) * basin_scale).astype(jnp.float32)
    peak_change = jnp.max(jnp.abs(sat_new - sat_old))
    return basin_totals, column_balance, peak_change
```

```python
import jax
import jax.numpy as jnp
from jax import lax
from jax.experimental import pallas as pl
from jax.experimental.pallas import tpu as pltpu
from jax.sharding import PartitionSpec as P

SUB = 512
CH = 8
ZB = 16
MESH = pl.DeviceIdType.MESH
BF = jnp.bfloat16
F32 = jnp.float32
NT = (((1,), (1,)), ((), ()))


def split(f):
    high = f.astype(BF)
    return high, (f - high.astype(F32)).astype(BF)


def face_flow(p, k, pn, kn):
    return (k * kn) / (k + kn) * (p - pn)


def wait_all(ref, sem):
    pltpu.make_async_copy(ref, ref, sem).wait()


def make_kernel(ngx, ngy, scale):
    n = ngx * ngy

    def kernel(
        thick, labels, outlet, sn_h, so_h, po_h, ss_h, p_h, k_h, et_h,
        out, bal, top,
        sn, so, po, ss, et, p, k, depth, g, a, oh, tot, edge, halo, peak, peaks_y, peaks_x,
        pieces, own, sem_pk, sem_rest, halo_send, halo_recv, rs_send, rs_recv, ag_send, ag_recv,
        pk_send, pk_recv,
    ):
        layers, cx, cy = sn_h.shape
        chunks = cx // CH
        gx = lax.axis_index("gx")
        gy = lax.axis_index("gy")
        me = gx * ngy + gy
        barrier = pltpu.get_barrier_semaphore()

        def peer(d):
            other = lax.rem(me + d, n)
            return other, (other // ngy, lax.rem(other, ngy))

        @pl.loop(1, n)
        def _(d):
            pl.semaphore_signal(barrier, inc=1, device_id=peer(d)[1], device_id_type=MESH)

        @pl.loop(0, layers)
        def _(z):
            for i, (src, dst) in enumerate(((p_h, p), (k_h, k))):
                pltpu.make_async_copy(src.at[z], dst.at[pl.ds(0, cx), z, :], sem_pk.at[i]).start()

        rest = ((sn_h, sn), (so_h, so), (po_h, po), (ss_h, ss), (et_h, et))

        @pl.loop(0, chunks)
        def _(c):
            for r in range(CH):
                for i, (src, dst) in enumerate(rest):
                    x = c * CH + r
                    pltpu.make_async_copy(src.at[:, x, :], dst.at[x], sem_rest.at[i, c]).start()

        for z in range(layers):
            depth[pl.ds(z, 1), :] = jnp.full((1, cy), thick[z], F32)
        p[cx] = jnp.zeros((layers, cy), F32)
        k[cx] = jnp.zeros((layers, cy), F32)
        g[...] = jnp.zeros_like(g)
        peak[...] = jnp.zeros_like(peak)
        tot[...] = jnp.zeros_like(tot)
        lane = lax.broadcasted_iota(jnp.int32, (ZB, cy), 1)
        inner = lane > 0
        iota = lax.broadcasted_iota(jnp.int32, (256, cy), 0).astype(F32).astype(BF)
        one = jnp.ones((16, cy), BF)
        zero = jnp.zeros((16, cy), BF)

        def write_onehot(lab, col):
            high = lab >= 256
            low = jnp.where(high, lab - 256, lab).astype(F32)
            low = jnp.broadcast_to(low, (16, cy)).astype(BF)
            high = jnp.broadcast_to(jnp.where(high, 1.0, 0.0), (16, cy)).astype(BF)
            for r in range(16):
                e = jnp.where(iota[r * 16 : (r + 1) * 16] == low, one, zero)
                eh = e * high
                oh[pl.ds(r * 16, 16), col] = e - eh
                oh[pl.ds(256 + r * 16, 16), col] = eh

        wait_all(p.at[pl.ds(0, cx)], sem_pk.at[0])
        wait_all(k.at[pl.ds(0, cx)], sem_pk.at[1])

        lanes = lax.broadcasted_iota(jnp.int32, (layers, cy), 1)

        def take(x, carry):
            first, last = lanes == x, lanes == x + cx
            res = []
            for ref, acc in zip((p, k), carry):
                v = ref[x]
                acc = jnp.where(first, pltpu.roll(v, x, 1), acc)
                res.append(jnp.where(last, pltpu.roll(v, x + cx + 1, 1), acc))
            return tuple(res)

        e0 = jnp.zeros((layers, cy), F32)
        ep, ek = lax.fori_loop(0, cx, take, (e0, e0))
        edge[0] = ep
        edge[1] = ek

        def chunk(c):
            for i, (_, dst) in enumerate(rest):
                wait_all(dst.at[pl.ds(c * CH, CH)], sem_rest.at[i, c])

            @pl.loop(0, CH)
            def _(i):
                x = c * CH + i
                col = pl.ds(pl.multiple_of(i * cy, cy), cy)
                write_onehot(labels[pl.ds(x, 1), :], col)
                mask = outlet[pl.ds(x, 1), :].astype(F32)
                sums = [jnp.zeros((8, cy), F32)] * 4
                top_here = peak[...]
                for zb in range(layers // ZB):
                    zs = pl.ds(zb * ZB, ZB)
                    d = depth[zs, :]
                    pc, kc = p[x, zs, :], k[x, zs, :]
                    gn = face_flow(p[x + 1, zs, :], kc, pc, k[x + 1, zs, :])
                    gp = g[zs, :]
                    g[zs, :] = gn
                    h = face_flow(pc, kc, pltpu.roll(pc, 1, 1), pltpu.roll(kc, 1, 1))
                    h = jnp.where(inner, h, 0.0)
                    flux = (d + d) * (gp - gn + h - pltpu.roll(h, cy - 1, 1))
                    snv, pov = sn[x, zs, :], po[x, zs, :]
                    dif = snv - so[x, zs, :]
                    water = d * snv * (pov + ss[x, zs, :] * pc)
                    change = d * pov * dif
                    uptake = d * et[x, zs, :]
                    big = jnp.abs(dif)
                    top_here = jnp.maximum(top_here, jnp.maximum(big[:8], big[8:]))
                    for q, f in enumerate((water, change, uptake, flux)):
                        sums[q] = sums[q] + (f[:8] + f[8:])
                        high, low = split(f * mask if q == 3 else f)
                        a[pl.ds(q * layers + zb * ZB, ZB), col] = high
                        a[pl.ds((4 + q) * layers + zb * ZB, ZB), col] = low
                peak[...] = top_here
                for q in range(4):
                    bal[q, pl.ds(x, 1), :] = jnp.sum(sums[q], axis=0, keepdims=True)

            r = lax.dot_general(a[...], oh[...], NT, preferred_element_type=F32)
            tot[...] += r[: 4 * layers] + r[4 * layers :]

        half = chunks // 2

        @pl.loop(0, half)
        def _(c):
            chunk(c)

        pl.semaphore_wait(barrier, n - 1)

        def halo_copy(src, slot, ox, oy):
            to = (lax.rem(gx + ox + ngx, ngx), lax.rem(gy + oy + ngy, ngy))
            return pltpu.make_async_remote_copy(
                src_ref=src, dst_ref=halo.at[slot], send_sem=halo_send.at[slot],
                recv_sem=halo_recv.at[slot], device_id=to, device_id_type=MESH,
            )

        halos = []
        for i, ref in enumerate((p, k)):
            halos.append(halo_copy(ref.at[cx - 1], i, 1, 0))
            halos.append(halo_copy(ref.at[0], 2 + i, -1, 0))
            halos.append(halo_copy(edge.at[i], 4 + i, 0, 1))
            halos.append(halo_copy(edge.at[i], 6 + i, 0, -1))
        for h in halos:
            h.start()

        @pl.loop(half, chunks)
        def _(c):
            chunk(c)

        for h in halos:
            h.wait()
        left = lanes < cx
        ly = jnp.concatenate([labels[...]] * 2, axis=0).astype(F32).T
        oy = jnp.concatenate([outlet[...]] * 2, axis=0).astype(F32).T
        first = lax.broadcasted_iota(jnp.int32, (1, cy), 1) < cx
        lab_y = jnp.where(first, ly[:1], ly[cy - 1 :]).astype(jnp.int32)
        out_y = jnp.where(first, oy[:1], oy[cy - 1 :])
        d2 = depth[...] + depth[...]
        py = jnp.where(left, pltpu.roll(halo[4], cx, 1), pltpu.roll(halo[6], cx, 1))
        ky = jnp.where(left, pltpu.roll(halo[5], cx, 1), pltpu.roll(halo[7], cx, 1))
        inside = jnp.where(left, jnp.where(gy > 0, 1.0, 0.0), jnp.where(gy < ngy - 1, 1.0, 0.0))
        borders = (
            (p[0], k[0], halo[0], halo[1] * jnp.where(gx > 0, 1.0, 0.0), labels[:1, :], outlet[:1, :].astype(F32)),
            (
                p[cx - 1], k[cx - 1], halo[2], halo[3] * jnp.where(gx < ngx - 1, 1.0, 0.0),
                labels[cx - 1 :, :], outlet[cx - 1 :, :].astype(F32),
            ),
            (edge[0], edge[1], py, ky * inside, lab_y, out_y),
        )
        for i, (pc, kc, pn, kn, lab, mask) in enumerate(borders):
            f = d2 * face_flow(pc, kc, pn, kn)
            col = pl.ds(i * cy, cy)
            write_onehot(lab, col)
            high, low = split(f * mask)
            a[pl.ds(0, layers), col] = high
            a[pl.ds(layers, layers), col] = low
            f = jnp.sum(f, axis=0, keepdims=True)
            if i < 2:
                x = i * (cx - 1)
                bal[3, x : x + 1, :] += f
            else:
                ft = jnp.broadcast_to(f, (8, cy)).T
                at = lax.broadcasted_iota(jnp.int32, (cx, cy), 1)
                low_side = jnp.where(at == 0, jnp.broadcast_to(ft[:cx, :1], (cx, cy)), 0.0)
                high_side = jnp.where(at == cy - 1, jnp.broadcast_to(ft[cx:, :1], (cx, cy)), 0.0)
                bal[3] += low_side + high_side
        r = lax.dot_general(
            a[: 2 * layers, : 3 * cy], oh[:, : 3 * cy], NT, preferred_element_type=F32
        )
        tot[pl.ds(3 * layers, layers), :] += r[:layers] + r[layers:]

        def peak_copy(src, dst, send, recv, to):
            return pltpu.make_async_remote_copy(
                src_ref=src, dst_ref=dst, send_sem=send, recv_sem=recv, device_id=to, device_id_type=MESH
            )

        @pl.loop(1, ngy)
        def _(d):
            to = (gx, lax.rem(gy + d, ngy))
            peak_copy(peak, peaks_y.at[d - 1], pk_send.at[0], pk_recv.at[0], to).start()

        def tile(ref, owner):
            per_row = SUB // 128
            row = pl.multiple_of(owner // per_row * 8, 8)
            colt = pl.multiple_of(lax.rem(owner, per_row) * 128, 128)
            return ref.at[pl.ds(row, 8), pl.ds(colt, 128)]

        @pl.loop(1, n)
        def _(d):
            other, to = peer(d)
            peak_copy(tile(tot, other), pieces.at[d - 1], rs_send, rs_recv, to).start()

        wait_all(peaks_y, pk_recv.at[0])
        wait_all(peaks_y, pk_send.at[0])
        best = peak[...]
        for d in range(ngy - 1):
            best = jnp.maximum(best, peaks_y[d])
        peak[...] = best

        @pl.loop(1, ngx)
        def _(d):
            to = (lax.rem(gx + d, ngx), gy)
            peak_copy(peak, peaks_x.at[d - 1], pk_send.at[1], pk_recv.at[1], to).start()

        wait_all(pieces, rs_recv)
        total = tile(tot, me)[...]
        for d in range(n - 1):
            total = total + pieces[d]
        own[...] = total * scale

        @pl.loop(1, n)
        def _(d):
            _, to = peer(d)
            peak_copy(own, tile(out, me), ag_send, ag_recv, to).start()

        tile(out, me)[...] = own[...]
        wait_all(peaks_x, pk_recv.at[1])
        wait_all(peaks_x, pk_send.at[1])
        best = peak[...]
        for d in range(ngx - 1):
            best = jnp.maximum(best, peaks_x[d])
        top[0] = jnp.max(best)
        wait_all(pieces, rs_send)
        wait_all(pieces, ag_recv)
        wait_all(pieces, ag_send)

    return kernel


def solution(mesh):
    ngx, ngy = mesh.shape["gx"], mesh.shape["gy"]
    n = ngx * ngy

    def on_device(sat_new, sat_old, porosity, spec_storage, pressure, conduct, et_rate, thickness, labels, outlet):
        layers, cx, cy = sat_new.shape
        scale = layers * SUB / (ngx * cx * ngy * cy)
        field = pltpu.VMEM((cx, layers, cy), F32)
        longer = pltpu.VMEM((cx + 1, layers, cy), F32)
        sheet = pltpu.VMEM((layers, cy), F32)
        dma = pltpu.SemaphoreType.DMA
        vm = pl.BlockSpec(memory_space=pltpu.VMEM)
        out, bal, top = pl.pallas_call(
            make_kernel(ngx, ngy, scale),
            out_shape=(
                jax.ShapeDtypeStruct((4 * layers, SUB), F32),
                jax.ShapeDtypeStruct((4, cx, cy), F32),
                jax.ShapeDtypeStruct((1,), F32),
            ),
            in_specs=[pl.BlockSpec(memory_space=pltpu.SMEM), vm, vm] + [pl.BlockSpec(memory_space=pl.ANY)] * 7,
            out_specs=(vm, vm, pl.BlockSpec(memory_space=pltpu.SMEM)),
            scratch_shapes=[
                field, field, field, field, field, longer, longer,
                sheet,
                sheet,
                pltpu.VMEM((8 * layers, CH * cy), BF),
                pltpu.VMEM((SUB, CH * cy), BF),
                pltpu.VMEM((4 * layers, SUB), F32),
                pltpu.VMEM((2, layers, cy), F32),
                pltpu.VMEM((8, layers, cy), F32),
                pltpu.VMEM((8, cy), F32),
                pltpu.VMEM((ngy - 1, 8, cy), F32),
                pltpu.VMEM((ngx - 1, 8, cy), F32),
                pltpu.VMEM((n - 1, 8, 128), F32),
                pltpu.VMEM((8, 128), F32),
                dma((2,)), dma((5, cx // CH)), dma((8,)), dma((8,)), dma, dma, dma, dma, dma((2,)), dma((2,)),
            ],
            compiler_params=pltpu.CompilerParams(
                collective_id=0, has_side_effects=True, vmem_limit_bytes=60 << 20
            ),
            name="balance",
        )(thickness, labels, outlet, sat_new, sat_old, porosity, spec_storage, pressure, conduct, et_rate)
        return out.reshape(4, layers, SUB), bal, top.reshape(())

    cells = P(None, "gx", "gy")
    return jax.shard_map(
        on_device,
        mesh=mesh,
        in_specs=(cells,) * 7 + (P(), P("gx", "gy"), P("gx", "gy")),
        out_specs=(P(), cells, P()),
        check_vma=False,
    )
```

```python
import jax
import jax.numpy as jnp
from jax import lax
from jax.experimental import pallas as pl
from jax.experimental.pallas import tpu as pltpu
from jax.sharding import PartitionSpec as P

SUB = 512
NP = 4
ZB = 16
MESH = pl.DeviceIdType.MESH
BF = jnp.bfloat16
F32 = jnp.float32
NT = (((1,), (1,)), ((), ()))


def split(f):
    high = f.astype(BF)
    return high, (f - high.astype(F32)).astype(BF)


def face_flow(p, k, pn, kn):
    return (k * kn) / (k + kn) * (p - pn)


def wait_all(ref, sem):
    pltpu.make_async_copy(ref, ref, sem).wait()


def make_kernel(ngx, ngy, scale):
    chips_y = ngy // 2
    n = ngx * ngy

    def kernel(
        thick_h, labels_h, outlet_h, sn_h, so_h, po_h, ss_h, p_h, k_h, et_h,
        out, bal_h, top,
        thick, labels, outlet, sn, so, po, ss, et, p, k, depth, g, a0, a1, oh0, oh1, tot, half, whole, bal,
        edge, halo, peak, peaks_y, peaks_x, pieces, own,
        sem_small, sem_pk, sem_rest, halo_send, halo_recv, pair_send, pair_recv,
        rs_send, rs_recv, ag_send, ag_recv, pk_send, pk_recv, sem_out,
    ):
        layers, cx, cy = sn_h.shape
        per = 2 * NP
        turns = cx // per
        gx = lax.axis_index("gx")
        gy = lax.axis_index("gy")
        chip = gy // 2
        core = gy - chip * 2
        barrier = pltpu.get_barrier_semaphore()

        def wrap(v, m):
            return jnp.where(v >= m, v - m, v)

        smalls = ((thick_h, thick), (labels_h, labels), (outlet_h, outlet))
        for i, (src, dst) in enumerate(smalls):
            pltpu.make_async_copy(src, dst, sem_small.at[i]).start()

        @pl.loop(0, layers)
        def _(z):
            for i, (src, dst) in enumerate(((p_h, p), (k_h, k))):
                pltpu.make_async_copy(src.at[z], dst.at[pl.ds(0, cx), z, :], sem_pk.at[i]).start()

        rest = ((sn_h, sn), (so_h, so), (po_h, po), (ss_h, ss), (et_h, et))

        @pl.loop(0, turns)
        def _(c):
            for r in range(per):
                for i, (src, dst) in enumerate(rest):
                    x = c * per + r
                    pltpu.make_async_copy(src.at[:, x, :], dst.at[x], sem_rest.at[i, c]).start()

        chips = [wrap(chip + d, chips_y) for d in range(chips_y)]

        def each_chip(f):
            for d in range(1, chips_y):
                f(d - 1, gx, chips[d])

            @pl.loop(1, ngx)
            def _(i):
                at = wrap(gx + i, ngx)
                for d in range(chips_y):
                    f(i * chips_y + d - 1, at, chips[d])

        def greet(to):
            pl.semaphore_signal(barrier, inc=1, device_id=to, device_id_type=MESH)

        partner = (gx, chip * 2 + 1 - core)
        greet(partner)
        each_chip(lambda i, x, z: greet((x, z * 2 + core)))
        for d in range(1, chips_y):
            greet((gx, chips[d] * 2 + 1 - core))

        for (src, dst), i in zip(smalls, range(3)):
            pltpu.make_async_copy(src, dst, sem_small.at[i]).wait()
        for z in range(layers):
            depth[pl.ds(z, 1), :] = jnp.full((1, cy), thick[z], F32)
        p[cx] = jnp.zeros((layers, cy), F32)
        k[cx] = jnp.zeros((layers, cy), F32)
        g[...] = jnp.zeros_like(g)
        peak[...] = jnp.zeros_like(peak)
        tot[...] = jnp.zeros_like(tot)
        a1[...] = jnp.zeros_like(a1)
        oh1[...] = jnp.zeros_like(oh1)
        lane = lax.broadcasted_iota(jnp.int32, (ZB, cy), 1)
        inner = lane > 0
        iota = lax.broadcasted_iota(jnp.int32, (256, cy), 0).astype(F32).astype(BF)
        one = jnp.ones((16, cy), BF)
        zero = jnp.zeros((16, cy), BF)

        def write_onehot(oh, lab, col):
            high = lab >= 256
            low = jnp.where(high, lab - 256, lab).astype(F32)
            low = jnp.broadcast_to(low, (16, cy)).astype(BF)
            high = jnp.broadcast_to(jnp.where(high, 1.0, 0.0), (16, cy)).astype(BF)
            for r in range(16):
                e = jnp.where(iota[r * 16 : (r + 1) * 16] == low, one, zero)
                eh = e * high
                oh[r * 16 : r * 16 + 16, col] = e - eh
                oh[256 + r * 16 : 272 + r * 16, col] = eh

        wait_all(p.at[pl.ds(0, cx)], sem_pk.at[0])
        wait_all(k.at[pl.ds(0, cx)], sem_pk.at[1])

        lanes = lax.broadcasted_iota(jnp.int32, (layers, cy), 1)

        def take(x, carry):
            first, last = lanes == x, lanes == x + cx
            res = []
            for ref, acc in zip((p, k), carry):
                v = ref[x]
                acc = jnp.where(first, pltpu.roll(v, x, 1), acc)
                res.append(jnp.where(last, pltpu.roll(v, x + cx + 1, 1), acc))
            return tuple(res)

        e0 = jnp.zeros((layers, cy), F32)
        ep, ek = lax.fori_loop(0, cx, take, (e0, e0))
        edge[0] = ep
        edge[1] = ek

        def fields(x, a, oh, j):
            col = slice(j * cy, (j + 1) * cy)
            write_onehot(oh, labels[pl.ds(x, 1), :], col)
            mask = outlet[pl.ds(x, 1), :].astype(F32)
            sums = [jnp.zeros((8, cy), F32)] * 4
            top_here = peak[...]
            for zb in range(layers // ZB):
                zs = pl.ds(zb * ZB, ZB)
                d = depth[zs, :]
                pc, kc = p[x, zs, :], k[x, zs, :]
                gn = face_flow(p[x + 1, zs, :], kc, pc, k[x + 1, zs, :])
                gp = g[zs, :]
                g[zs, :] = gn
                h = face_flow(pc, kc, pltpu.roll(pc, 1, 1), pltpu.roll(kc, 1, 1))
                h = jnp.where(inner, h, 0.0)
                flux = (d + d) * (gp - gn + h - pltpu.roll(h, cy - 1, 1))
                snv, pov = sn[x, zs, :], po[x, zs, :]
                dif = snv - so[x, zs, :]
                water = d * snv * (pov + ss[x, zs, :] * pc)
                change = d * pov * dif
                uptake = d * et[x, zs, :]
                big = jnp.abs(dif)
                top_here = jnp.maximum(top_here, jnp.maximum(big[:8], big[8:]))
                for q, f in enumerate((water, change, uptake, flux)):
                    sums[q] = sums[q] + (f[:8] + f[8:])
                    high, low = split(f * mask if q == 3 else f)
                    r0 = q * layers + zb * ZB
                    a[r0 : r0 + ZB, col] = high
                    a[4 * layers + r0 : 4 * layers + r0 + ZB, col] = low
            peak[...] = top_here
            for q in range(4):
                bal[q, pl.ds(x, 1), :] = jnp.sum(sums[q], axis=0, keepdims=True)

        def product(a, oh):
            r = lax.dot_general(a[...], oh[...], NT, preferred_element_type=F32)
            tot[...] += r[: 4 * layers] + r[4 * layers :]

        def turns_of(begin, end):
            @pl.loop(begin, end)
            def _(c):
                for i, (_, dst) in enumerate(rest):
                    wait_all(dst.at[pl.ds(c * per, per)], sem_rest.at[i, c])
                product(a1, oh1)
                for j in range(NP):
                    fields(c * per + j, a0, oh0, j)
                product(a0, oh0)
                for j in range(NP):
                    fields(c * per + NP + j, a1, oh1, j)

        def send(src, dst, send_sem, recv_sem, to):
            copy = pltpu.make_async_remote_copy(
                src_ref=src, dst_ref=dst, send_sem=send_sem, recv_sem=recv_sem, device_id=to, device_id_type=MESH
            )
            copy.start()
            return copy

        turns_of(0, turns // 2)
        pl.semaphore_wait(barrier, (ngx + 1) * chips_y - 1)

        x_next, x_last = wrap(gx + 1, ngx), wrap(gx + ngx - 1, ngx)
        y_next, y_last = wrap(gy + 1, ngy), wrap(gy + ngy - 1, ngy)
        halos = []
        for i, ref in enumerate((p, k)):
            for slot, src, to in (
                (i, ref.at[cx - 1], (x_next, gy)),
                (2 + i, ref.at[0], (x_last, gy)),
                (4 + i, edge.at[i], (gx, y_next)),
                (6 + i, edge.at[i], (gx, y_last)),
            ):
                halos.append(send(src, halo.at[slot], halo_send.at[slot], halo_recv.at[slot], to))

        turns_of(turns // 2, turns)
        product(a1, oh1)

        chips8 = [wrap(gy + d, ngy) for d in range(1, ngy)]
        for d in range(ngy - 1):
            send(peak, peaks_y.at[d], pk_send.at[0], pk_recv.at[0], (gx, chips8[d]))

        for h in halos:
            h.wait()
        left = lanes < cx
        ly = jnp.concatenate([labels[...]] * 2, axis=0).astype(F32).T
        oy = jnp.concatenate([outlet[...]] * 2, axis=0).astype(F32).T
        first = lax.broadcasted_iota(jnp.int32, (1, cy), 1) < cx
        lab_y = jnp.where(first, ly[:1], ly[cy - 1 :]).astype(jnp.int32)
        out_y = jnp.where(first, oy[:1], oy[cy - 1 :])
        d2 = depth[...] + depth[...]
        py = jnp.where(left, pltpu.roll(halo[4], cx, 1), pltpu.roll(halo[6], cx, 1))
        ky = jnp.where(left, pltpu.roll(halo[5], cx, 1), pltpu.roll(halo[7], cx, 1))
        inside = jnp.where(left, jnp.where(gy > 0, 1.0, 0.0), jnp.where(gy < ngy - 1, 1.0, 0.0))
        borders = (
            (p[0], k[0], halo[0], halo[1] * jnp.where(gx > 0, 1.0, 0.0), labels[:1, :], outlet[:1, :].astype(F32)),
            (
                p[cx - 1], k[cx - 1], halo[2], halo[3] * jnp.where(gx < ngx - 1, 1.0, 0.0),
                labels[cx - 1 :, :], outlet[cx - 1 :, :].astype(F32),
            ),
            (edge[0], edge[1], py, ky * inside, lab_y, out_y),
        )
        for i, (pc, kc, pn, kn, lab, mask) in enumerate(borders):
            f = d2 * face_flow(pc, kc, pn, kn)
            col = slice(i * cy, (i + 1) * cy)
            write_onehot(oh0, lab, col)
            high, low = split(f * mask)
            a0[:layers, col] = high
            a0[layers : 2 * layers, col] = low
            f = jnp.sum(f, axis=0, keepdims=True)
            if i < 2:
                x = i * (cx - 1)
                bal[3, x : x + 1, :] += f
            else:
                ft = jnp.broadcast_to(f, (8, cy)).T
                at = lax.broadcasted_iota(jnp.int32, (cx, cy), 1)
                low_side = jnp.where(at == 0, jnp.broadcast_to(ft[:cx, :1], (cx, cy)), 0.0)
                high_side = jnp.where(at == cy - 1, jnp.broadcast_to(ft[cx:, :1], (cx, cy)), 0.0)
                bal[3] += low_side + high_side
        r = lax.dot_general(
            a0[: 2 * layers, : 3 * cy], oh0[:, : 3 * cy], NT, preferred_element_type=F32
        )
        tot[pl.ds(3 * layers, layers), :] += r[:layers] + r[layers:]

        rows = 2 * layers
        mine, theirs = (pl.multiple_of(v * rows, rows) for v in (core, 1 - core))
        pair = send(tot.at[pl.ds(theirs, rows), :], half, pair_send.at[0], pair_recv.at[0], partner)
        bal_copy = pltpu.make_async_copy(bal, bal_h, sem_out.at[0])
        bal_copy.start()

        wait_all(peaks_y, pk_recv.at[0])
        wait_all(peaks_y, pk_send.at[0])
        best = peak[...]
        for d in range(ngy - 1):
            best = jnp.maximum(best, peaks_y[d])
        peak[...] = best

        pair.wait()
        tot[pl.ds(mine, rows), :] += half[...]

        def tile(ref, x, z):
            return ref.at[
                pl.ds(pl.multiple_of(core * rows + x * 8, 8), 8), pl.ds(pl.multiple_of(z * 128, 128), 128)
            ]

        each_chip(lambda i, x, z: send(tile(tot, x, z), pieces.at[i], rs_send, rs_recv, (x, z * 2 + core)))

        @pl.loop(1, ngx)
        def _(d):
            send(peak, peaks_x.at[d - 1], pk_send.at[1], pk_recv.at[1], (wrap(gx + d, ngx), gy))

        wait_all(pieces, rs_recv)
        terms = [tile(tot, gx, chip)[...]] + [pieces[d] for d in range(n // 2 - 1)]
        while len(terms) > 1:
            terms = [a + b for a, b in zip(terms[::2], terms[1::2])] + terms[len(terms) // 2 * 2 :]
        own[...] = terms[0] * scale

        here = tile(whole, gx, chip)
        each_chip(lambda i, x, z: send(own, here, ag_send, ag_recv, (x, z * 2 + core)))
        here[...] = own[...]
        wait_all(peaks_x, pk_recv.at[1])
        wait_all(peaks_x, pk_send.at[1])
        best = peak[...]
        for d in range(ngx - 1):
            best = jnp.maximum(best, peaks_x[d])
        top[0] = jnp.max(best)
        bal_copy.wait()
        wait_all(pieces, rs_send)
        wait_all(pieces, ag_recv)
        done = whole.at[pl.ds(mine, rows), :]
        pair = send(done, out.at[pl.ds(mine, rows), :], pair_send.at[1], pair_recv.at[1], partner)
        out_copy = pltpu.make_async_copy(done, out.at[pl.ds(mine, rows), :], sem_out.at[1])
        out_copy.start()
        wait_all(pieces, ag_send)
        out_copy.wait()
        pair.wait()

    return kernel


def solution(mesh):
    ngx, ngy = mesh.shape["gx"], mesh.shape["gy"]
    n = ngx * ngy

    def on_device(sat_new, sat_old, porosity, spec_storage, pressure, conduct, et_rate, thickness, labels, outlet):
        layers, cx, cy = sat_new.shape
        scale = layers * SUB / (ngx * cx * ngy * cy)
        field = pltpu.VMEM((cx, layers, cy), F32)
        longer = pltpu.VMEM((cx + 1, layers, cy), F32)
        sheet = pltpu.VMEM((layers, cy), F32)
        dma = pltpu.SemaphoreType.DMA
        anywhere = pl.BlockSpec(memory_space=pl.ANY)
        out, bal, top = pl.pallas_call(
            make_kernel(ngx, ngy, scale),
            out_shape=(
                jax.ShapeDtypeStruct((4 * layers, SUB), F32),
                jax.ShapeDtypeStruct((4, cx, cy), F32),
                jax.ShapeDtypeStruct((1,), F32),
            ),
            in_specs=[anywhere] * 10,
            out_specs=(anywhere, anywhere, pl.BlockSpec(memory_space=pltpu.SMEM)),
            scratch_shapes=[
                pltpu.SMEM((layers,), F32),
                pltpu.VMEM((cx, cy), jnp.int32),
                pltpu.VMEM((cx, cy), jnp.int32),
                field, field, field, field, field, longer, longer,
                sheet,
                sheet,
                pltpu.VMEM((8 * layers, NP * cy), BF),
                pltpu.VMEM((8 * layers, NP * cy), BF),
                pltpu.VMEM((SUB, NP * cy), BF),
                pltpu.VMEM((SUB, NP * cy), BF),
                pltpu.VMEM((4 * layers, SUB), F32),
                pltpu.VMEM((2 * layers, SUB), F32),
                pltpu.VMEM((4 * layers, SUB), F32),
                pltpu.VMEM((4, cx, cy), F32),
                pltpu.VMEM((2, layers, cy), F32),
                pltpu.VMEM((8, layers, cy), F32),
                pltpu.VMEM((8, cy), F32),
                pltpu.VMEM((ngy - 1, 8, cy), F32),
                pltpu.VMEM((ngx - 1, 8, cy), F32),
                pltpu.VMEM((n // 2 - 1, 8, 128), F32),
                pltpu.VMEM((8, 128), F32),
                dma((3,)), dma((2,)), dma((5, cx // (2 * NP))), dma((8,)), dma((8,)), dma((2,)), dma((2,)),
                dma, dma, dma, dma, dma((2,)), dma((2,)), dma((2,)),
            ],
            compiler_params=pltpu.CompilerParams(
                collective_id=0, has_side_effects=True, vmem_limit_bytes=60 << 20
            ),
            name="balance",
        )(thickness, labels, outlet, sat_new, sat_old, porosity, spec_storage, pressure, conduct, et_rate)
        return out.reshape(4, layers, SUB), bal, top.reshape(())

    cells = P(None, "gx", "gy")
    return jax.shard_map(
        on_device,
        mesh=mesh,
        in_specs=(cells,) * 7 + (P(), P("gx", "gy"), P("gx", "gy")),
        out_specs=(P(), cells, P()),
        check_vma=False,
    )
```

```python
import jax
import jax.numpy as jnp
from jax import lax
from jax.experimental import pallas as pl
from jax.experimental.pallas import tpu as pltpu
from jax.sharding import PartitionSpec as P

SUB = 512
NP = 4
ZB = 16
MESH = pl.DeviceIdType.MESH
BF = jnp.bfloat16
F32 = jnp.float32
NT = (((1,), (1,)), ((), ()))


def split(f):
    high = f.astype(BF)
    return high, (f - high.astype(F32)).astype(BF)


def face_flow(p, k, pn, kn):
    return (k * kn) / (k + kn) * (p - pn)


def wait_all(ref, sem):
    pltpu.make_async_copy(ref, ref, sem).wait()


def make_kernel(ngx, ngy, scale):
    chips_y = ngy // 2
    n = ngx * ngy

    def kernel(
        thick_h, labels_h, outlet_h, sn_h, so_h, po_h, ss_h, p_h, k_h, et_h,
        out, bal_h, top,
        thick, labels, outlet, sn, so, po, ss, et, p, k, depth, g, a0, a1, oh0, oh1, tot, half, bal,
        edge, halo, peak, peaks_y, peaks_x, pieces, own,
        sem_small, sem_pk, sem_rest, halo_send, halo_recv, pair_send, pair_recv,
        rs_send, rs_recv, ag_send, ag_recv, pk_send, pk_recv, sem_out,
    ):
        layers, cx, cy = sn_h.shape
        per = 2 * NP
        turns = cx // per
        gx = lax.axis_index("gx")
        gy = lax.axis_index("gy")
        chip = gy // 2
        core = gy - chip * 2
        barrier = pltpu.get_barrier_semaphore()

        def wrap(v, m):
            return jnp.where(v >= m, v - m, v)

        chips = [wrap(chip + d, chips_y) for d in range(chips_y)]

        def each_chip(f):
            for d in range(1, chips_y):
                f(d - 1, gx, chips[d])

            @pl.loop(1, ngx)
            def _(i):
                at = wrap(gx + i, ngx)
                for d in range(chips_y):
                    f(i * chips_y + d - 1, at, chips[d])

        def greet(to):
            pl.semaphore_signal(barrier, inc=1, device_id=to, device_id_type=MESH)

        partner = (gx, chip * 2 + 1 - core)
        greet(partner)
        each_chip(lambda i, x, z: greet((x, z * 2 + core)))
        for d in range(1, chips_y):
            greet((gx, chips[d] * 2 + 1 - core))

        smalls = ((thick_h, thick), (labels_h, labels), (outlet_h, outlet))
        for i, (src, dst) in enumerate(smalls):
            pltpu.make_async_copy(src, dst, sem_small.at[i]).start()

        @pl.loop(0, layers)
        def _(z):
            for i, (src, dst) in enumerate(((p_h, p), (k_h, k))):
                pltpu.make_async_copy(src.at[z], dst.at[pl.ds(0, cx), z, :], sem_pk.at[i]).start()

        rest = ((sn_h, sn), (so_h, so), (po_h, po), (ss_h, ss), (et_h, et))

        @pl.loop(0, turns)
        def _(c):
            for r in range(per):
                for i, (src, dst) in enumerate(rest):
                    x = c * per + r
                    pltpu.make_async_copy(src.at[:, x, :], dst.at[x], sem_rest.at[i, c]).start()

        for (src, dst), i in zip(smalls, range(3)):
            pltpu.make_async_copy(src, dst, sem_small.at[i]).wait()
        for z in range(layers):
            depth[pl.ds(z, 1), :] = jnp.full((1, cy), thick[z], F32)
        p[cx] = jnp.zeros((layers, cy), F32)
        k[cx] = jnp.zeros((layers, cy), F32)
        g[...] = jnp.zeros_like(g)
        peak[...] = jnp.zeros_like(peak)
        tot[...] = jnp.zeros_like(tot)
        a1[...] = jnp.zeros_like(a1)
        oh1[...] = jnp.zeros_like(oh1)
        lane = lax.broadcasted_iota(jnp.int32, (ZB, cy), 1)
        inner = lane > 0
        iota = lax.broadcasted_iota(jnp.int32, (256, cy), 0).astype(F32).astype(BF)
        one = jnp.ones((16, cy), BF)
        zero = jnp.zeros((16, cy), BF)

        def write_onehot(oh, lab, col):
            high = lab >= 256
            low = jnp.where(high, lab - 256, lab).astype(F32)
            low = jnp.broadcast_to(low, (16, cy)).astype(BF)
            high = jnp.broadcast_to(jnp.where(high, 1.0, 0.0), (16, cy)).astype(BF)
            for r in range(16):
                e = jnp.where(iota[r * 16 : (r + 1) * 16] == low, one, zero)
                eh = e * high
                oh[r * 16 : r * 16 + 16, col] = e - eh
                oh[256 + r * 16 : 272 + r * 16, col] = eh

        wait_all(p.at[pl.ds(0, cx)], sem_pk.at[0])
        wait_all(k.at[pl.ds(0, cx)], sem_pk.at[1])

        lanes = lax.broadcasted_iota(jnp.int32, (layers, cy), 1)

        def take(t, carry):
            for x in (4 * t, 4 * t + 1, 4 * t + 2, 4 * t + 3):
                first, last = lanes == x, lanes == x + cx
                res = []
                for ref, acc in zip((p, k), carry):
                    v = ref[x]
                    acc = jnp.where(first, pltpu.roll(v, x, 1), acc)
                    res.append(jnp.where(last, pltpu.roll(v, x + cx + 1, 1), acc))
                carry = tuple(res)
            return carry

        e0 = jnp.zeros((layers, cy), F32)
        ep, ek = lax.fori_loop(0, cx // 4, take, (e0, e0))
        edge[0] = ep
        edge[1] = ek

        def fields(x, a, oh, j):
            col = slice(j * cy, (j + 1) * cy)
            write_onehot(oh, labels[pl.ds(x, 1), :], col)
            mask = outlet[pl.ds(x, 1), :].astype(F32)
            sums = [jnp.zeros((8, cy), F32)] * 4
            top_here = peak[...]
            for zb in range(layers // ZB):
                zs = pl.ds(zb * ZB, ZB)
                d = depth[zs, :]
                pc, kc = p[x, zs, :], k[x, zs, :]
                gn = face_flow(p[x + 1, zs, :], kc, pc, k[x + 1, zs, :])
                gp = g[zs, :]
                g[zs, :] = gn
                h = face_flow(pc, kc, pltpu.roll(pc, 1, 1), pltpu.roll(kc, 1, 1))
                h = jnp.where(inner, h, 0.0)
                flux = (d + d) * (gp - gn + h - pltpu.roll(h, cy - 1, 1))
                snv, pov = sn[x, zs, :], po[x, zs, :]
                dif = snv - so[x, zs, :]
                water = d * snv * (pov + ss[x, zs, :] * pc)
                change = d * pov * dif
                uptake = d * et[x, zs, :]
                big = jnp.abs(dif)
                top_here = jnp.maximum(top_here, jnp.maximum(big[:8], big[8:]))
                for q, f in enumerate((water, change, uptake, flux)):
                    sums[q] = sums[q] + (f[:8] + f[8:])
                    high, low = split(f * mask if q == 3 else f)
                    r0 = q * layers + zb * ZB
                    a[r0 : r0 + ZB, col] = high
                    a[4 * layers + r0 : 4 * layers + r0 + ZB, col] = low
            peak[...] = top_here
            for q in range(4):
                bal[q, pl.ds(x, 1), :] = jnp.sum(sums[q], axis=0, keepdims=True)

        def product(a, oh):
            r = lax.dot_general(a[...], oh[...], NT, preferred_element_type=F32)
            tot[...] += r[: 4 * layers] + r[4 * layers :]

        def turns_of(begin, end):
            @pl.loop(begin, end)
            def _(c):
                for i, (_, dst) in enumerate(rest):
                    wait_all(dst.at[pl.ds(c * per, per)], sem_rest.at[i, c])
                product(a1, oh1)
                for j in range(NP):
                    fields(c * per + j, a0, oh0, j)
                product(a0, oh0)
                for j in range(NP):
                    fields(c * per + NP + j, a1, oh1, j)

        def send(src, dst, send_sem, recv_sem, to):
            copy = pltpu.make_async_remote_copy(
                src_ref=src, dst_ref=dst, send_sem=send_sem, recv_sem=recv_sem, device_id=to, device_id_type=MESH
            )
            copy.start()
            return copy

        turns_of(0, turns // 2)
        pl.semaphore_wait(barrier, (ngx + 1) * chips_y - 1)

        x_next, x_last = wrap(gx + 1, ngx), wrap(gx + ngx - 1, ngx)
        y_next, y_last = wrap(gy + 1, ngy), wrap(gy + ngy - 1, ngy)
        halos = []
        for i, ref in enumerate((p, k)):
            for slot, src, to in (
                (i, ref.at[cx - 1], (x_next, gy)),
                (2 + i, ref.at[0], (x_last, gy)),
                (4 + i, edge.at[i], (gx, y_next)),
                (6 + i, edge.at[i], (gx, y_last)),
            ):
                halos.append(send(src, halo.at[slot], halo_send.at[slot], halo_recv.at[slot], to))

        turns_of(turns // 2, turns)
        product(a1, oh1)

        chips8 = [wrap(gy + d, ngy) for d in range(1, ngy)]
        for d in range(ngy - 1):
            send(peak, peaks_y.at[d], pk_send.at[0], pk_recv.at[0], (gx, chips8[d]))

        for h in halos:
            h.wait()
        left = lanes < cx
        ly = jnp.concatenate([labels[...]] * 2, axis=0).astype(F32).T
        oy = jnp.concatenate([outlet[...]] * 2, axis=0).astype(F32).T
        first = lax.broadcasted_iota(jnp.int32, (1, cy), 1) < cx
        lab_y = jnp.where(first, ly[:1], ly[cy - 1 :]).astype(jnp.int32)
        out_y = jnp.where(first, oy[:1], oy[cy - 1 :])
        d2 = depth[...] + depth[...]
        py = jnp.where(left, pltpu.roll(halo[4], cx, 1), pltpu.roll(halo[6], cx, 1))
        ky = jnp.where(left, pltpu.roll(halo[5], cx, 1), pltpu.roll(halo[7], cx, 1))
        inside = jnp.where(left, jnp.where(gy > 0, 1.0, 0.0), jnp.where(gy < ngy - 1, 1.0, 0.0))
        borders = (
            (p[0], k[0], halo[0], halo[1] * jnp.where(gx > 0, 1.0, 0.0), labels[:1, :], outlet[:1, :].astype(F32)),
            (
                p[cx - 1], k[cx - 1], halo[2], halo[3] * jnp.where(gx < ngx - 1, 1.0, 0.0),
                labels[cx - 1 :, :], outlet[cx - 1 :, :].astype(F32),
            ),
            (edge[0], edge[1], py, ky * inside, lab_y, out_y),
        )
        for i, (pc, kc, pn, kn, lab, mask) in enumerate(borders):
            f = d2 * face_flow(pc, kc, pn, kn)
            col = slice(i * cy, (i + 1) * cy)
            write_onehot(oh0, lab, col)
            high, low = split(f * mask)
            a0[:layers, col] = high
            a0[layers : 2 * layers, col] = low
            f = jnp.sum(f, axis=0, keepdims=True)
            if i < 2:
                x = i * (cx - 1)
                bal[3, x : x + 1, :] += f
            else:
                ft = jnp.broadcast_to(f, (8, cy)).T
                at = lax.broadcasted_iota(jnp.int32, (cx, cy), 1)
                low_side = jnp.where(at == 0, jnp.broadcast_to(ft[:cx, :1], (cx, cy)), 0.0)
                high_side = jnp.where(at == cy - 1, jnp.broadcast_to(ft[cx:, :1], (cx, cy)), 0.0)
                bal[3] += low_side + high_side
        r = lax.dot_general(
            a0[: 2 * layers, : 3 * cy], oh0[:, : 3 * cy], NT, preferred_element_type=F32
        )
        tot[pl.ds(3 * layers, layers), :] += r[:layers] + r[layers:]

        rows = 2 * layers
        mine, theirs = (pl.multiple_of(v * rows, rows) for v in (core, 1 - core))
        pair = send(tot.at[pl.ds(theirs, rows), :], half, pair_send.at[0], pair_recv.at[0], partner)
        bal_copy = pltpu.make_async_copy(bal, bal_h, sem_out.at[0])
        bal_copy.start()

        wait_all(peaks_y, pk_recv.at[0])
        wait_all(peaks_y, pk_send.at[0])
        best = peak[...]
        for d in range(ngy - 1):
            best = jnp.maximum(best, peaks_y[d])
        peak[...] = best

        pair.wait()
        tot[pl.ds(mine, rows), :] += half[...]

        def tile(ref, x, z):
            return ref.at[
                pl.ds(pl.multiple_of(core * rows + x * 8, 8), 8), pl.ds(pl.multiple_of(z * 128, 128), 128)
            ]

        each_chip(lambda i, x, z: send(tile(tot, x, z), pieces.at[i], rs_send, rs_recv, (x, z * 2 + core)))

        @pl.loop(1, ngx)
        def _(d):
            send(peak, peaks_x.at[d - 1], pk_send.at[1], pk_recv.at[1], (wrap(gx + d, ngx), gy))

        wait_all(pieces, rs_recv)
        terms = [tile(tot, gx, chip)[...]] + [pieces[d] for d in range(n // 2 - 1)]
        while len(terms) > 1:
            terms = [a + b for a, b in zip(terms[::2], terms[1::2])] + terms[len(terms) // 2 * 2 :]
        own[...] = terms[0] * scale

        here = tile(out, gx, chip)
        each_chip(lambda i, x, z: send(own, here, ag_send, ag_recv, (x, z * 2 + core)))
        own_copy = pltpu.make_async_copy(own, here, sem_out.at[1])
        own_copy.start()
        wait_all(peaks_x, pk_recv.at[1])
        wait_all(peaks_x, pk_send.at[1])
        best = peak[...]
        for d in range(ngx - 1):
            best = jnp.maximum(best, peaks_x[d])
        top[0] = jnp.max(best)
        bal_copy.wait()
        wait_all(pieces, rs_send)
        wait_all(pieces, ag_recv)
        own_copy.wait()
        done = out.at[pl.ds(mine, rows), :]
        pair = send(done, done, pair_send.at[1], pair_recv.at[1], partner)
        wait_all(pieces, ag_send)
        pair.wait()

    return kernel


def solution(mesh):
    ngx, ngy = mesh.shape["gx"], mesh.shape["gy"]
    n = ngx * ngy

    def on_device(sat_new, sat_old, porosity, spec_storage, pressure, conduct, et_rate, thickness, labels, outlet):
        layers, cx, cy = sat_new.shape
        scale = layers * SUB / (ngx * cx * ngy * cy)
        field = pltpu.VMEM((cx, layers, cy), F32)
        longer = pltpu.VMEM((cx + 1, layers, cy), F32)
        sheet = pltpu.VMEM((layers, cy), F32)
        dma = pltpu.SemaphoreType.DMA
        anywhere = pl.BlockSpec(memory_space=pl.ANY)
        out, bal, top = pl.pallas_call(
            make_kernel(ngx, ngy, scale),
            out_shape=(
                jax.ShapeDtypeStruct((4 * layers, SUB), F32),
                jax.ShapeDtypeStruct((4, cx, cy), F32),
                jax.ShapeDtypeStruct((1,), F32),
            ),
            in_specs=[pl.BlockSpec(memory_space=pltpu.HBM)] * 10,
            out_specs=(anywhere, anywhere, pl.BlockSpec(memory_space=pltpu.SMEM)),
            scratch_shapes=[
                pltpu.SMEM((layers,), F32),
                pltpu.VMEM((cx, cy), jnp.int32),
                pltpu.VMEM((cx, cy), jnp.int32),
                field, field, field, field, field, longer, longer,
                sheet,
                sheet,
                pltpu.VMEM((8 * layers, NP * cy), BF),
                pltpu.VMEM((8 * layers, NP * cy), BF),
                pltpu.VMEM((SUB, NP * cy), BF),
                pltpu.VMEM((SUB, NP * cy), BF),
                pltpu.VMEM((4 * layers, SUB), F32),
                pltpu.VMEM((2 * layers, SUB), F32),
                pltpu.VMEM((4, cx, cy), F32),
                pltpu.VMEM((2, layers, cy), F32),
                pltpu.VMEM((8, layers, cy), F32),
                pltpu.VMEM((8, cy), F32),
                pltpu.VMEM((ngy - 1, 8, cy), F32),
                pltpu.VMEM((ngx - 1, 8, cy), F32),
                pltpu.VMEM((n // 2 - 1, 8, 128), F32),
                pltpu.VMEM((8, 128), F32),
                dma((3,)), dma((2,)), dma((5, cx // (2 * NP))), dma((8,)), dma((8,)), dma((2,)), dma((2,)),
                dma, dma, dma, dma, dma((2,)), dma((2,)), dma((2,)),
            ],
            compiler_params=pltpu.CompilerParams(
                collective_id=0, has_side_effects=True, vmem_limit_bytes=48 << 20
            ),
            name="balance",
        )(*(
            pltpu.with_memory_space_constraint(v, pltpu.HBM)
            for v in (thickness, labels, outlet, sat_new, sat_old, porosity, spec_storage, pressure, conduct, et_rate)
        ))
        return out.reshape(4, layers, SUB), bal, top.reshape(())

    cells = P(None, "gx", "gy")
    return jax.shard_map(
        on_device,
        mesh=mesh,
        in_specs=(cells,) * 7 + (P(), P("gx", "gy"), P("gx", "gy")),
        out_specs=(P(), cells, P()),
        check_vma=False,
    )
```

```python
import jax
import jax.numpy as jnp
from jax import lax
from jax.experimental import pallas as pl
from jax.experimental.pallas import tpu as pltpu
from jax.sharding import PartitionSpec as P

SUB = 512
NP = 4
ZB = 16
PARTS = (8, 24, 32)
MESH = pl.DeviceIdType.MESH
BF = jnp.bfloat16
F32 = jnp.float32


def split(f):
    high = f.astype(BF)
    return high, (f - high.astype(F32)).astype(BF)


def face_flow(p, k, pn, kn):
    return (k * kn) / (k + kn) * (p - pn)


def wait_all(ref, sem):
    pltpu.make_async_copy(ref, ref, sem).wait()


def make_kernel(ngx, ngy, scale):
    chips_y = ngy // 2
    n = ngx * ngy

    def kernel(
        thick_h, labels_h, outlet_h, sn_h, so_h, po_h, ss_h, p_h, k_h, et_h,
        out, bal_h, top,
        thick, labels, outlet, sn, so, po, ss, et, p, k, depth, g, a0, a1, oh0, oh1, tot, half, bal,
        edge, halo, peak, peak_y, peaks_y, peaks_x, pieces, own,
        sem_small, sem_pk, sem_rest, halo_send, halo_recv, pair_send, pair_recv,
        rs_send, rs_recv, ag_send, ag_recv, pk_send, pk_recv, sem_out, main, edges,
    ):
        layers, cx, cy = sn_h.shape
        per = 2 * NP
        turns = cx // per
        early = turns // 2
        gx = lax.axis_index("gx")
        gy = lax.axis_index("gy")
        chip = gy // 2
        core = gy - chip * 2
        barrier = pltpu.get_barrier_semaphore()

        def wrap(v, m):
            return jnp.where(v >= m, v - m, v)

        chips = [wrap(chip + d, chips_y) for d in range(chips_y)]

        def each_chip(f):
            for d in range(1, chips_y):
                f(d - 1, gx, chips[d])

            @pl.loop(1, ngx)
            def _(i):
                at = wrap(gx + i, ngx)
                for d in range(chips_y):
                    f(i * chips_y + d - 1, at, chips[d])

        def greet(to):
            pl.semaphore_signal(barrier, inc=1, device_id=to, device_id_type=MESH)

        smalls = ((thick_h, thick), (labels_h, labels), (outlet_h, outlet))
        for i, (src, dst) in enumerate(smalls):
            pltpu.make_async_copy(src, dst, sem_small.at[i]).start()

        for i, (src, dst) in enumerate(((p_h, p), (k_h, k))):

            @pl.loop(0, layers // 4)
            def _(t, i=i, src=src, dst=dst):
                for r in range(4):
                    z = t * 4 + r
                    pltpu.make_async_copy(src.at[z], dst.at[pl.ds(0, cx), z, :], sem_pk.at[i]).start()

        partner = (gx, chip * 2 + 1 - core)
        greet(partner)
        each_chip(lambda i, x, z: greet((x, z * 2 + core)))
        for d in range(1, chips_y):
            greet((gx, chips[d] * 2 + 1 - core))

        rest = ((sn_h, sn), (so_h, so), (po_h, po), (ss_h, ss), (et_h, et))

        @pl.loop(0, PARTS[0])
        def _(x):
            for i, (src, dst) in enumerate(rest):
                pltpu.make_async_copy(src.at[:, x, :], dst.at[x], sem_rest.at[i, 0]).start()

        for part in range(1, len(PARTS)):
            rows_x = pl.ds(sum(PARTS[:part]), PARTS[part])

            @pl.loop(0, layers)
            def _(z, part=part, rows_x=rows_x):
                for i, (src, dst) in enumerate(rest):
                    pltpu.make_async_copy(src.at[z, rows_x, :], dst.at[rows_x, z, :], sem_rest.at[i, part]).start()

        for (src, dst), i in zip(smalls, range(3)):
            pltpu.make_async_copy(src, dst, sem_small.at[i]).wait()
        for z in range(layers):
            depth[pl.ds(z, 1), :] = jnp.full((1, cy), thick[z], F32)
        p[cx] = jnp.zeros((layers, cy), F32)
        k[cx] = jnp.zeros((layers, cy), F32)
        g[...] = jnp.zeros_like(g)
        peak[...] = jnp.zeros_like(peak)
        a1[...] = jnp.zeros_like(a1)
        oh1[...] = jnp.zeros_like(oh1)
        iota = lax.broadcasted_iota(jnp.int32, (256, cy), 0).astype(F32).astype(BF)
        zero = jnp.zeros((16, cy), BF)

        def write_onehot(oh, lab, col):
            high = lab >= 256
            low = jnp.where(high, lab - 256, lab).astype(F32)
            low = jnp.broadcast_to(low, (16, cy)).astype(BF)
            lower = jnp.broadcast_to(jnp.where(high, 0.0, 1.0), (16, cy)).astype(BF)
            upper = jnp.broadcast_to(jnp.where(high, 1.0, 0.0), (16, cy)).astype(BF)
            for r in range(16):
                hit = iota[r * 16 : (r + 1) * 16] == low
                oh[r * 16 : r * 16 + 16, col] = jnp.where(hit, lower, zero)
                oh[256 + r * 16 : 272 + r * 16, col] = jnp.where(hit, upper, zero)

        lanes = lax.broadcasted_iota(jnp.int32, (layers, cy), 1)
        for i, ref in enumerate((p, k)):
            wait_all(ref.at[pl.ds(0, cx)], sem_pk.at[i])

            def take(t, acc, ref=ref):
                for r in range(8):
                    x = t * 8 + r
                    v = ref[x]
                    acc = jnp.where(lanes == x, pltpu.roll(v, x, 1), acc)
                    acc = jnp.where(lanes == x + cx, pltpu.roll(v, x + cx + 1, 1), acc)
                return acc

            edge[i] = lax.fori_loop(0, cx // 8, take, jnp.zeros((layers, cy), F32))

        def fields(x, a, oh, j):
            col = slice(j * cy, (j + 1) * cy)
            write_onehot(oh, labels[pl.ds(x, 1), :], col)
            mask = outlet[pl.ds(x, 1), :].astype(F32)
            sums = [jnp.zeros((8, cy), F32)] * 4
            top_here = peak[...]
            for zb in range(layers // ZB):
                zs = pl.ds(zb * ZB, ZB)
                d = depth[zs, :]
                pc, kc = p[x, zs, :], k[x, zs, :]
                gn = face_flow(p[x + 1, zs, :], kc, pc, k[x + 1, zs, :])
                gp = g[zs, :]
                g[zs, :] = gn
                h = face_flow(pc, kc, pltpu.roll(pc, 1, 1), pltpu.roll(kc, 1, 1))
                flux = (d + d) * (gp - gn + h - pltpu.roll(h, cy - 1, 1))
                snv, pov = sn[x, zs, :], po[x, zs, :]
                dif = snv - so[x, zs, :]
                water = d * snv * (pov + ss[x, zs, :] * pc)
                change = d * pov * dif
                uptake = d * et[x, zs, :]
                big = jnp.abs(dif)
                top_here = jnp.maximum(top_here, jnp.maximum(big[:8], big[8:]))
                for q, f in enumerate((water, change, uptake, flux)):
                    sums[q] = sums[q] + (f[:8] + f[8:])
                    high, low = split(f * mask if q == 3 else f)
                    r0 = q * layers + zb * ZB
                    a[r0 : r0 + ZB, col] = high
                    a[4 * layers + r0 : 4 * layers + r0 + ZB, col] = low
            peak[...] = top_here
            for q in range(4):
                bal[q, pl.ds(x, 1), :] = jnp.sum(sums[q], axis=0, keepdims=True)

        def product(a, oh, rows, sums, width):
            for t in range(width // 256):
                col = slice(t * 256, t * 256 + 256)
                for m in (0, 1):
                    pltpu.matmul_push_rhs(
                        oh[m * 256 : m * 256 + 256, col], staging_register=t % 2, mxu_index=m, transpose=True
                    )
                for m in (0, 1):
                    pltpu.matmul_acc_lhs(sums[m], a[:rows, col], load_staged_rhs=t % 2)
                    pltpu.matmul_acc_lhs(sums[m], a[rows : 2 * rows, col])

        def turns_of(begin, end):
            @pl.loop(begin, end)
            def _(c):
                for part, size in enumerate(PARTS):
                    begin_x = sum(PARTS[:part])
                    if begin <= begin_x // per < end:

                        @pl.when(c == begin_x // per)
                        def _(part=part, size=size, begin_x=begin_x):
                            for i, (_, dst) in enumerate(rest):
                                wait_all(dst.at[pl.ds(begin_x, size)], sem_rest.at[i, part])

                product(a1, oh1, 4 * layers, main, NP * cy)
                for j in range(NP):
                    fields(c * per + j, a0, oh0, j)
                product(a0, oh0, 4 * layers, main, NP * cy)
                for j in range(NP):
                    fields(c * per + NP + j, a1, oh1, j)

        def send(src, dst, send_sem, recv_sem, to):
            copy = pltpu.make_async_remote_copy(
                src_ref=src, dst_ref=dst, send_sem=send_sem, recv_sem=recv_sem, device_id=to, device_id_type=MESH
            )
            copy.start()
            return copy

        turns_of(0, early)
        pl.semaphore_wait(barrier, (ngx + 1) * chips_y - 1)

        x_next, x_last = wrap(gx + 1, ngx), wrap(gx + ngx - 1, ngx)
        y_next, y_last = wrap(gy + 1, ngy), wrap(gy + ngy - 1, ngy)
        halos = []
        for i, ref in enumerate((p, k)):
            for slot, src, to in (
                (i, ref.at[cx - 1], (x_next, gy)),
                (2 + i, ref.at[0], (x_last, gy)),
                (4 + i, edge.at[i], (gx, y_next)),
                (6 + i, edge.at[i], (gx, y_last)),
            ):
                halos.append(send(src, halo.at[slot], halo_send.at[slot], halo_recv.at[slot], to))

        turns_of(early, turns)

        peak[...] = jnp.broadcast_to(jnp.max(peak[...], axis=0, keepdims=True), (8, cy))

        @pl.loop(1, ngx)
        def _(d):
            send(peak.at[:1, :], peaks_x.at[d - 1], pk_send.at[0], pk_recv.at[0], (wrap(gx + d, ngx), gy))

        for h in halos:
            h.wait()
        product(a1, oh1, 4 * layers, main, NP * cy)
        left = lanes < cx
        ly = jnp.concatenate([labels[...]] * 2, axis=0).astype(F32).T
        oy = jnp.concatenate([outlet[...]] * 2, axis=0).astype(F32).T
        first = lax.broadcasted_iota(jnp.int32, (1, cy), 1) < cx
        lab_y = jnp.where(first, ly[:1], ly[cy - 1 :]).astype(jnp.int32)
        out_y = jnp.where(first, oy[:1], oy[cy - 1 :])
        d2 = depth[...] + depth[...]
        py = jnp.where(left, pltpu.roll(halo[4], cx, 1), pltpu.roll(halo[6], cx, 1))
        ky = jnp.where(left, pltpu.roll(halo[5], cx, 1), pltpu.roll(halo[7], cx, 1))
        inside = jnp.where(left, jnp.where(gy > 0, 1.0, 0.0), jnp.where(gy < ngy - 1, 1.0, 0.0))
        borders = (
            (p[0], k[0], halo[0], halo[1] * jnp.where(gx > 0, 1.0, 0.0), labels[:1, :], outlet[:1, :].astype(F32)),
            (
                p[cx - 1], k[cx - 1], halo[2], halo[3] * jnp.where(gx < ngx - 1, 1.0, 0.0),
                labels[cx - 1 :, :], outlet[cx - 1 :, :].astype(F32),
            ),
            (edge[0], edge[1], py, ky * inside, lab_y, out_y),
        )
        for i, (pc, kc, pn, kn, lab, mask) in enumerate(borders):
            f = face_flow(pc, kc, pn, kn)
            if i == 2:
                f = f - face_flow(pc, kc, pltpu.roll(pc, cx, 1), pltpu.roll(kc, cx, 1))
            f = d2 * f
            col = slice(i * cy, (i + 1) * cy)
            write_onehot(oh0, lab, col)
            high, low = split(f * mask)
            a0[:layers, col] = high
            a0[layers : 2 * layers, col] = low
            f = jnp.sum(f, axis=0, keepdims=True)
            if i < 2:
                x = i * (cx - 1)
                bal[3, x : x + 1, :] += f
            else:
                ft = jnp.broadcast_to(f, (8, cy)).T
                at = lax.broadcasted_iota(jnp.int32, (cx, cy), 1)
                low_side = jnp.where(at == 0, jnp.broadcast_to(ft[:cx, :1], (cx, cy)), 0.0)
                high_side = jnp.where(at == cy - 1, jnp.broadcast_to(ft[cx:, :1], (cx, cy)), 0.0)
                bal[3] += low_side + high_side
        a0[: 2 * layers, 3 * cy : 4 * cy] = jnp.zeros((2 * layers, cy), BF)
        product(a0, oh0, layers, edges, 4 * cy)
        for m in (0, 1):
            col = slice(m * 256, m * 256 + 256)
            r = pltpu.matmul_pop(main[m])
            tot[: 3 * layers, col] = r[: 3 * layers]
            tot[3 * layers :, col] = r[3 * layers :] + pltpu.matmul_pop(edges[m])

        rows = 2 * layers
        mine, theirs = (pl.multiple_of(v * rows, rows) for v in (core, 1 - core))
        pair = send(tot.at[pl.ds(theirs, rows), :], half, pair_send.at[0], pair_recv.at[0], partner)
        bal_copy = pltpu.make_async_copy(bal, bal_h, sem_out.at[0])
        bal_copy.start()

        pair.wait()
        tot[pl.ds(mine, rows), :] += half[...]

        def tile(ref, x, z):
            return ref.at[
                pl.ds(pl.multiple_of(core * rows + x * 8, 8), 8), pl.ds(pl.multiple_of(z * 128, 128), 128)
            ]

        each_chip(lambda i, x, z: send(tile(tot, x, z), pieces.at[i], rs_send, rs_recv, (x, z * 2 + core)))

        wait_all(pieces, rs_recv)
        terms = [tile(tot, gx, chip)[...]] + [pieces[d] for d in range(n // 2 - 1)]
        while len(terms) > 1:
            terms = [a + b for a, b in zip(terms[::2], terms[1::2])] + terms[len(terms) // 2 * 2 :]
        own[...] = terms[0] * scale

        here = tile(out, gx, chip)
        each_chip(lambda i, x, z: send(own, here, ag_send, ag_recv, (x, z * 2 + core)))
        own_copy = pltpu.make_async_copy(own, here, sem_out.at[1])
        own_copy.start()
        wait_all(peaks_x, pk_recv.at[0])
        wait_all(peaks_x, pk_send.at[0])
        best = peak[:1, :]
        for d in range(ngx - 1):
            best = jnp.maximum(best, peaks_x[d])
        peak_y[...] = best
        for d in range(1, ngy):
            send(peak_y, peaks_y.at[d - 1], pk_send.at[1], pk_recv.at[1], (gx, wrap(gy + d, ngy)))
        bal_copy.wait()
        wait_all(pieces, rs_send)
        wait_all(pieces, ag_recv)
        own_copy.wait()
        done = out.at[pl.ds(mine, rows), :]
        pair = send(done, done, pair_send.at[1], pair_recv.at[1], partner)
        wait_all(pieces, ag_send)
        wait_all(peaks_y, pk_recv.at[1])
        wait_all(peaks_y, pk_send.at[1])
        for d in range(ngy - 1):
            best = jnp.maximum(best, peaks_y[d])
        top[0] = jnp.max(best)
        pair.wait()

    def with_sums(*refs):
        layers = refs[3].shape[0]

        def body(main_0, main_1, edge_0, edge_1):
            for r in (main_0, main_1, edge_0, edge_1):
                pltpu.matmul_pop(r)
            kernel(*refs, (main_0, main_1), (edge_0, edge_1))

        pl.run_scoped(
            body,
            pltpu.ACC(0)((4 * layers, 256), F32), pltpu.ACC(1)((4 * layers, 256), F32),
            pltpu.ACC(0)((layers, 256), F32), pltpu.ACC(1)((layers, 256), F32),
        )

    return with_sums


def solution(mesh):
    ngx, ngy = mesh.shape["gx"], mesh.shape["gy"]
    n = ngx * ngy

    def on_device(sat_new, sat_old, porosity, spec_storage, pressure, conduct, et_rate, thickness, labels, outlet):
        layers, cx, cy = sat_new.shape
        scale = layers * SUB / (ngx * cx * ngy * cy)
        field = pltpu.VMEM((cx, layers, cy), F32)
        longer = pltpu.VMEM((cx + 1, layers, cy), F32)
        sheet = pltpu.VMEM((layers, cy), F32)
        dma = pltpu.SemaphoreType.DMA
        anywhere = pl.BlockSpec(memory_space=pl.ANY)
        out, bal, top = pl.pallas_call(
            make_kernel(ngx, ngy, scale),
            out_shape=(
                jax.ShapeDtypeStruct((4 * layers, SUB), F32),
                jax.ShapeDtypeStruct((4, cx, cy), F32),
                jax.ShapeDtypeStruct((1,), F32),
            ),
            in_specs=[pl.BlockSpec(memory_space=pltpu.HBM)] * 10,
            out_specs=(anywhere, anywhere, pl.BlockSpec(memory_space=pltpu.SMEM)),
            scratch_shapes=[
                pltpu.SMEM((layers,), F32),
                pltpu.VMEM((cx, cy), jnp.int32),
                pltpu.VMEM((cx, cy), jnp.int32),
                field, field, field, field, field, longer, longer,
                sheet,
                sheet,
                pltpu.VMEM((8 * layers, NP * cy), BF),
                pltpu.VMEM((8 * layers, NP * cy), BF),
                pltpu.VMEM((SUB, NP * cy), BF),
                pltpu.VMEM((SUB, NP * cy), BF),
                pltpu.VMEM((4 * layers, SUB), F32),
                pltpu.VMEM((2 * layers, SUB), F32),
                pltpu.VMEM((4, cx, cy), F32),
                pltpu.VMEM((2, layers, cy), F32),
                pltpu.VMEM((8, layers, cy), F32),
                pltpu.VMEM((8, cy), F32),
                pltpu.VMEM((1, cy), F32),
                pltpu.VMEM((ngy - 1, 1, cy), F32),
                pltpu.VMEM((ngx - 1, 1, cy), F32),
                pltpu.VMEM((n // 2 - 1, 8, 128), F32),
                pltpu.VMEM((8, 128), F32),
                dma((3,)), dma((2,)), dma((5, len(PARTS))), dma((8,)), dma((8,)), dma((2,)), dma((2,)),
                dma, dma, dma, dma, dma((2,)), dma((2,)), dma((2,)),
            ],
            compiler_params=pltpu.CompilerParams(
                collective_id=0, has_side_effects=True, vmem_limit_bytes=48 << 20
            ),
            name="balance",
        )(*(
            pltpu.with_memory_space_constraint(v, pltpu.HBM)
            for v in (thickness, labels, outlet, sat_new, sat_old, porosity, spec_storage, pressure, conduct, et_rate)
        ))
        return out.reshape(4, layers, SUB), bal, top.reshape(())

    cells = P(None, "gx", "gy")
    return jax.shard_map(
        on_device,
        mesh=mesh,
        in_specs=(cells,) * 7 + (P(), P("gx", "gy"), P("gx", "gy")),
        out_specs=(P(), cells, P()),
        check_vma=False,
    )
```

```python
import jax
import jax.numpy as jnp
from jax import lax
from jax.experimental import pallas as pl
from jax.experimental.pallas import tpu as pltpu
from jax.sharding import PartitionSpec as P

SUB = 512
NP = 4
ZB = 16
PARTS = (8, 24, 32)
MESH = pl.DeviceIdType.MESH
BF = jnp.bfloat16
F32 = jnp.float32


def split(f):
    high = f.astype(BF)
    return high, (f - high.astype(F32)).astype(BF)


def face_flow(p, k, pn, kn):
    return (k * kn) / (k + kn) * (p - pn)


def wait_all(ref, sem):
    pltpu.make_async_copy(ref, ref, sem).wait()


def make_kernel(ngx, ngy, scale):
    chips_y = ngy // 2
    n = ngx * ngy

    def kernel(
        thick_h, labels_h, outlet_h, sn_h, so_h, po_h, ss_h, p_h, k_h, et_h,
        out, bal_h, top,
        thick, labels, outlet, sn, so, po, ss, et, p, k, depth, g, a0, a1, oh0, oh1, tot, half, bal,
        edge, halo, peak, peak_y, peaks_y, peaks_x, pieces, own,
        sem_small, sem_pk, sem_rest, halo_send, halo_recv, pair_send, pair_recv,
        rs_send, rs_recv, ag_send, ag_recv, pk_send, pk_recv, sem_out, main, edges,
    ):
        layers, cx, cy = sn_h.shape
        per = 2 * NP
        turns = cx // per
        early = turns * 3 // 8
        gx = lax.axis_index("gx")
        gy = lax.axis_index("gy")
        chip = gy // 2
        core = gy - chip * 2
        barrier = pltpu.get_barrier_semaphore()

        def wrap(v, m):
            return jnp.where(v >= m, v - m, v)

        chips = [wrap(chip + d, chips_y) for d in range(chips_y)]

        def each_chip(f):
            order = sorted(range(chips_y), key=lambda d: -min(d, chips_y - d))
            far = ngx * 3 // 8
            for begin, end in ((far, ngx), (1, far)):

                @pl.loop(begin, end)
                def _(i):
                    at = wrap(gx + i, ngx)
                    for d in order:
                        f(i * chips_y + d - 1, at, chips[d])

            for d in range(1, chips_y):
                f(d - 1, gx, chips[d])

        def greet(to):
            pl.semaphore_signal(barrier, inc=1, device_id=to, device_id_type=MESH)

        smalls = ((thick_h, thick), (labels_h, labels), (outlet_h, outlet))
        for i, (src, dst) in enumerate(smalls):
            pltpu.make_async_copy(src, dst, sem_small.at[i]).start()

        for i, (src, dst) in enumerate(((p_h, p), (k_h, k))):

            @pl.loop(0, layers // 16)
            def _(t, i=i, src=src, dst=dst):
                for r in range(16):
                    z = t * 16 + r
                    pltpu.make_async_copy(src.at[z], dst.at[pl.ds(0, cx), z, :], sem_pk.at[i]).start()

        rest = ((sn_h, sn), (so_h, so), (po_h, po), (ss_h, ss), (et_h, et))

        for x in range(PARTS[0]):
            for i, (src, dst) in enumerate(rest):
                pltpu.make_async_copy(src.at[:, x, :], dst.at[x], sem_rest.at[i, 0]).start()

        partner = (gx, chip * 2 + 1 - core)
        greet(partner)
        each_chip(lambda i, x, z: greet((x, z * 2 + core)))
        for d in range(1, chips_y):
            greet((gx, chips[d] * 2 + 1 - core))

        for part in range(1, len(PARTS)):
            rows_x = pl.ds(sum(PARTS[:part]), PARTS[part])

            @pl.loop(0, layers // 8)
            def _(t, part=part, rows_x=rows_x):
                for r in range(8):
                    z = t * 8 + r
                    for i, (src, dst) in enumerate(rest):
                        pltpu.make_async_copy(src.at[z, rows_x, :], dst.at[rows_x, z, :], sem_rest.at[i, part]).start()

        for (src, dst), i in zip(smalls, range(3)):
            pltpu.make_async_copy(src, dst, sem_small.at[i]).wait()
        for z in range(layers):
            depth[pl.ds(z, 1), :] = jnp.full((1, cy), thick[z], F32)
        p[cx] = jnp.zeros((layers, cy), F32)
        k[cx] = jnp.zeros((layers, cy), F32)
        g[...] = jnp.zeros_like(g)
        peak[...] = jnp.zeros_like(peak)
        a1[...] = jnp.zeros_like(a1)
        oh1[...] = jnp.zeros_like(oh1)
        iota = lax.broadcasted_iota(jnp.int32, (256, cy), 0).astype(F32).astype(BF)
        zero = jnp.zeros((16, cy), BF)

        def write_onehot(oh, lab, col):
            high = lab >= 256
            low = jnp.where(high, lab - 256, lab).astype(F32)
            low = jnp.broadcast_to(low, (16, cy)).astype(BF)
            lower = jnp.broadcast_to(jnp.where(high, 0.0, 1.0), (16, cy)).astype(BF)
            upper = jnp.broadcast_to(jnp.where(high, 1.0, 0.0), (16, cy)).astype(BF)
            for r in range(16):
                hit = iota[r * 16 : (r + 1) * 16] == low
                oh[r * 16 : r * 16 + 16, col] = jnp.where(hit, lower, zero)
                oh[256 + r * 16 : 272 + r * 16, col] = jnp.where(hit, upper, zero)

        lanes = lax.broadcasted_iota(jnp.int32, (layers, cy), 1)
        for i, ref in enumerate((p, k)):
            wait_all(ref.at[pl.ds(0, cx)], sem_pk.at[i])

            def take(t, carry, ref=ref):
                low, high = carry
                for r in range(8):
                    x = t * 8 + r
                    v = pltpu.roll(ref[x], x + cx, 1)
                    low = jnp.where(lanes == x + cx, v, low)
                    high = jnp.where(lanes == x + cx - 1, v, high)
                return low, high

            low, high = lax.fori_loop(0, cx // 8, take, (jnp.zeros((layers, cy), F32),) * 2)
            edge[i] = jnp.where(lanes < cx, pltpu.roll(low, cx, 1), pltpu.roll(high, 1, 1))

        def fields(x, a, oh, j):
            col = slice(j * cy, (j + 1) * cy)
            write_onehot(oh, labels[pl.ds(x, 1), :], col)
            mask = outlet[pl.ds(x, 1), :].astype(F32)
            sums = [jnp.zeros((8, cy), F32)] * 4
            top_here = peak[...]
            for zb in range(layers // ZB):
                zs = pl.ds(zb * ZB, ZB)
                d = depth[zs, :]
                pc, kc = p[x, zs, :], k[x, zs, :]
                gn = face_flow(p[x + 1, zs, :], kc, pc, k[x + 1, zs, :])
                gp = g[zs, :]
                g[zs, :] = gn
                h = face_flow(pc, kc, pltpu.roll(pc, 1, 1), pltpu.roll(kc, 1, 1))
                flux = (d + d) * (gp - gn + h - pltpu.roll(h, cy - 1, 1))
                snv, pov = sn[x, zs, :], po[x, zs, :]
                dif = snv - so[x, zs, :]
                water = d * snv * (pov + ss[x, zs, :] * pc)
                change = d * pov * dif
                uptake = d * et[x, zs, :]
                big = jnp.abs(dif)
                top_here = jnp.maximum(top_here, jnp.maximum(big[:8], big[8:]))
                for q, f in enumerate((water, change, uptake, flux)):
                    sums[q] = sums[q] + (f[:8] + f[8:])
                    high, low = split(f * mask if q == 3 else f)
                    r0 = q * layers + zb * ZB
                    a[r0 : r0 + ZB, col] = high
                    a[4 * layers + r0 : 4 * layers + r0 + ZB, col] = low
            peak[...] = top_here
            for q in range(4):
                bal[q, pl.ds(x, 1), :] = jnp.sum(sums[q], axis=0, keepdims=True)

        def product(a, oh, rows, sums, width):
            for t in range(width // 256):
                col = slice(t * 256, t * 256 + 256)
                for m in (0, 1):
                    pltpu.matmul_push_rhs(
                        oh[m * 256 : m * 256 + 256, col], staging_register=t % 2, mxu_index=m, transpose=True
                    )
                for m in (0, 1):
                    pltpu.matmul_acc_lhs(sums[m], a[:rows, col], load_staged_rhs=t % 2)
                    pltpu.matmul_acc_lhs(sums[m], a[rows : 2 * rows, col])

        def turns_of(begin, end):
            @pl.loop(begin, end)
            def _(c):
                for part, size in enumerate(PARTS):
                    begin_x = sum(PARTS[:part])
                    if begin <= begin_x // per < end:

                        @pl.when(c == begin_x // per)
                        def _(part=part, size=size, begin_x=begin_x):
                            for i, (_, dst) in enumerate(rest):
                                wait_all(dst.at[pl.ds(begin_x, size)], sem_rest.at[i, part])

                product(a1, oh1, 4 * layers, main, NP * cy)
                for j in range(NP):
                    fields(c * per + j, a0, oh0, j)
                product(a0, oh0, 4 * layers, main, NP * cy)
                for j in range(NP):
                    fields(c * per + NP + j, a1, oh1, j)

        def send(src, dst, send_sem, recv_sem, to):
            copy = pltpu.make_async_remote_copy(
                src_ref=src, dst_ref=dst, send_sem=send_sem, recv_sem=recv_sem, device_id=to, device_id_type=MESH
            )
            copy.start()
            return copy

        turns_of(0, early)
        pl.semaphore_wait(barrier, (ngx + 1) * chips_y - 1)

        x_next, x_last = wrap(gx + 1, ngx), wrap(gx + ngx - 1, ngx)
        y_next, y_last = wrap(gy + 1, ngy), wrap(gy + ngy - 1, ngy)
        halos = []
        for i, ref in enumerate((p, k)):
            for slot, src, to in (
                (i, ref.at[cx - 1], (x_next, gy)),
                (2 + i, ref.at[0], (x_last, gy)),
                (4 + i, edge.at[i], (gx, y_next)),
                (6 + i, edge.at[i], (gx, y_last)),
            ):
                halos.append(send(src, halo.at[slot], halo_send.at[slot], halo_recv.at[slot], to))

        turns_of(early, turns)

        peak[...] = jnp.broadcast_to(jnp.max(peak[...], axis=0, keepdims=True), (8, cy))

        @pl.loop(1, ngx)
        def _(d):
            send(peak.at[:1, :], peaks_x.at[d - 1], pk_send.at[0], pk_recv.at[0], (wrap(gx + d, ngx), gy))

        for h in halos:
            h.wait()
        product(a1, oh1, 4 * layers, main, NP * cy)
        left = lanes < cx
        ly = jnp.concatenate([labels[...]] * 2, axis=0).astype(F32).T
        oy = jnp.concatenate([outlet[...]] * 2, axis=0).astype(F32).T
        first = lax.broadcasted_iota(jnp.int32, (1, cy), 1) < cx
        lab_y = jnp.where(first, ly[:1], ly[cy - 1 :]).astype(jnp.int32)
        out_y = jnp.where(first, oy[:1], oy[cy - 1 :])
        d2 = depth[...] + depth[...]
        py = jnp.where(left, pltpu.roll(halo[4], cx, 1), pltpu.roll(halo[6], cx, 1))
        ky = jnp.where(left, pltpu.roll(halo[5], cx, 1), pltpu.roll(halo[7], cx, 1))
        inside = jnp.where(left, jnp.where(gy > 0, 1.0, 0.0), jnp.where(gy < ngy - 1, 1.0, 0.0))
        borders = (
            (p[0], k[0], halo[0], halo[1] * jnp.where(gx > 0, 1.0, 0.0), labels[:1, :], outlet[:1, :].astype(F32)),
            (
                p[cx - 1], k[cx - 1], halo[2], halo[3] * jnp.where(gx < ngx - 1, 1.0, 0.0),
                labels[cx - 1 :, :], outlet[cx - 1 :, :].astype(F32),
            ),
            (edge[0], edge[1], py, ky * inside, lab_y, out_y),
        )
        for i, (pc, kc, pn, kn, lab, mask) in enumerate(borders):
            f = face_flow(pc, kc, pn, kn)
            if i == 2:
                f = f - face_flow(pc, kc, pltpu.roll(pc, cx, 1), pltpu.roll(kc, cx, 1))
            f = d2 * f
            col = slice(i * cy, (i + 1) * cy)
            write_onehot(oh0, lab, col)
            high, low = split(f * mask)
            a0[:layers, col] = high
            a0[layers : 2 * layers, col] = low
            f = jnp.sum(f, axis=0, keepdims=True)
            if i < 2:
                x = i * (cx - 1)
                bal[3, x : x + 1, :] += f
            else:
                ft = jnp.broadcast_to(f, (8, cy)).T
                at = lax.broadcasted_iota(jnp.int32, (cx, cy), 1)
                low_side = jnp.where(at == 0, jnp.broadcast_to(ft[:cx, :1], (cx, cy)), 0.0)
                high_side = jnp.where(at == cy - 1, jnp.broadcast_to(ft[cx:, :1], (cx, cy)), 0.0)
                bal[3] += low_side + high_side
        a0[: 2 * layers, 3 * cy : 4 * cy] = jnp.zeros((2 * layers, cy), BF)
        product(a0, oh0, layers, edges, 4 * cy)
        for m in (0, 1):
            col = slice(m * 256, m * 256 + 256)
            r = pltpu.matmul_pop(main[m])
            tot[: 3 * layers, col] = r[: 3 * layers]
            tot[3 * layers :, col] = r[3 * layers :] + pltpu.matmul_pop(edges[m])

        rows = 2 * layers
        mine, theirs = (pl.multiple_of(v * rows, rows) for v in (core, 1 - core))
        pair = send(tot.at[pl.ds(theirs, rows), :], half, pair_send.at[0], pair_recv.at[0], partner)
        bal_copy = pltpu.make_async_copy(bal, bal_h, sem_out.at[0])
        bal_copy.start()

        pair.wait()
        tot[pl.ds(mine, rows), :] += half[...]

        def tile(ref, x, z):
            return ref.at[
                pl.ds(pl.multiple_of(core * rows + x * 8, 8), 8), pl.ds(pl.multiple_of(z * 128, 128), 128)
            ]

        each_chip(lambda i, x, z: send(tile(tot, x, z), pieces.at[i], rs_send, rs_recv, (x, z * 2 + core)))

        wait_all(pieces, rs_recv)
        terms = [tile(tot, gx, chip)[...]] + [pieces[d] for d in range(n // 2 - 1)]
        while len(terms) > 1:
            terms = [a + b for a, b in zip(terms[::2], terms[1::2])] + terms[len(terms) // 2 * 2 :]
        own[...] = terms[0] * scale

        here = tile(out, gx, chip)
        each_chip(lambda i, x, z: send(own, here, ag_send, ag_recv, (x, z * 2 + core)))
        own_copy = pltpu.make_async_copy(own, here, sem_out.at[1])
        own_copy.start()
        wait_all(peaks_x, pk_recv.at[0])
        wait_all(peaks_x, pk_send.at[0])
        best = peak[:1, :]
        for d in range(ngx - 1):
            best = jnp.maximum(best, peaks_x[d])
        peak_y[...] = best
        for d in range(1, ngy):
            send(peak_y, peaks_y.at[d - 1], pk_send.at[1], pk_recv.at[1], (gx, wrap(gy + d, ngy)))
        bal_copy.wait()
        wait_all(pieces, rs_send)
        wait_all(pieces, ag_recv)
        own_copy.wait()
        done = out.at[pl.ds(mine, rows), :]
        pair = send(done, done, pair_send.at[1], pair_recv.at[1], partner)
        wait_all(pieces, ag_send)
        wait_all(peaks_y, pk_recv.at[1])
        wait_all(peaks_y, pk_send.at[1])
        for d in range(ngy - 1):
            best = jnp.maximum(best, peaks_y[d])
        top[0] = jnp.max(best)
        pair.wait()

    def with_sums(*refs):
        layers = refs[3].shape[0]

        def body(main_0, main_1, edge_0, edge_1):
            for r in (main_0, main_1, edge_0, edge_1):
                pltpu.matmul_pop(r)
            kernel(*refs, (main_0, main_1), (edge_0, edge_1))

        pl.run_scoped(
            body,
            pltpu.ACC(0)((4 * layers, 256), F32), pltpu.ACC(1)((4 * layers, 256), F32),
            pltpu.ACC(0)((layers, 256), F32), pltpu.ACC(1)((layers, 256), F32),
        )

    return with_sums


def solution(mesh):
    ngx, ngy = mesh.shape["gx"], mesh.shape["gy"]
    n = ngx * ngy

    def on_device(sat_new, sat_old, porosity, spec_storage, pressure, conduct, et_rate, thickness, labels, outlet):
        layers, cx, cy = sat_new.shape
        scale = layers * SUB / (ngx * cx * ngy * cy)
        field = pltpu.VMEM((cx, layers, cy), F32)
        longer = pltpu.VMEM((cx + 1, layers, cy), F32)
        sheet = pltpu.VMEM((layers, cy), F32)
        dma = pltpu.SemaphoreType.DMA
        anywhere = pl.BlockSpec(memory_space=pl.ANY)
        out, bal, top = pl.pallas_call(
            make_kernel(ngx, ngy, scale),
            out_shape=(
                jax.ShapeDtypeStruct((4 * layers, SUB), F32),
                jax.ShapeDtypeStruct((4, cx, cy), F32),
                jax.ShapeDtypeStruct((1,), F32),
            ),
            in_specs=[pl.BlockSpec(memory_space=pltpu.HBM)] * 10,
            out_specs=(anywhere, anywhere, pl.BlockSpec(memory_space=pltpu.SMEM)),
            scratch_shapes=[
                pltpu.SMEM((layers,), F32),
                pltpu.VMEM((cx, cy), jnp.int32),
                pltpu.VMEM((cx, cy), jnp.int32),
                field, field, field, field, field, longer, longer,
                sheet,
                sheet,
                pltpu.VMEM((8 * layers, NP * cy), BF),
                pltpu.VMEM((8 * layers, NP * cy), BF),
                pltpu.VMEM((SUB, NP * cy), BF),
                pltpu.VMEM((SUB, NP * cy), BF),
                pltpu.VMEM((4 * layers, SUB), F32),
                pltpu.VMEM((2 * layers, SUB), F32),
                pltpu.VMEM((4, cx, cy), F32),
                pltpu.VMEM((2, layers, cy), F32),
                pltpu.VMEM((8, layers, cy), F32),
                pltpu.VMEM((8, cy), F32),
                pltpu.VMEM((1, cy), F32),
                pltpu.VMEM((ngy - 1, 1, cy), F32),
                pltpu.VMEM((ngx - 1, 1, cy), F32),
                pltpu.VMEM((n // 2 - 1, 8, 128), F32),
                pltpu.VMEM((8, 128), F32),
                dma((3,)), dma((2,)), dma((5, len(PARTS))), dma((8,)), dma((8,)), dma((2,)), dma((2,)),
                dma, dma, dma, dma, dma((2,)), dma((2,)), dma((2,)),
            ],
            compiler_params=pltpu.CompilerParams(
                collective_id=0, has_side_effects=True, vmem_limit_bytes=48 << 20
            ),
            name="balance",
        )(*(
            pltpu.with_memory_space_constraint(v, pltpu.HBM)
            for v in (thickness, labels, outlet, sat_new, sat_old, porosity, spec_storage, pressure, conduct, et_rate)
        ))
        return out.reshape(4, layers, SUB), bal, top.reshape(())

    cells = P(None, "gx", "gy")
    return jax.shard_map(
        on_device,
        mesh=mesh,
        in_specs=(cells,) * 7 + (P(), P("gx", "gy"), P("gx", "gy")),
        out_specs=(P(), cells, P()),
        check_vma=False,
    )
```

```python
import jax
import jax.numpy as jnp
from jax import lax
from jax.experimental import pallas as pl
from jax.experimental.pallas import tpu as pltpu
from jax.sharding import PartitionSpec as P

SUB = 512
NP = 4
ZB = 16
PARTS = (8, 24, 32)
MESH = pl.DeviceIdType.MESH
BF = jnp.bfloat16
F32 = jnp.float32


def split(f):
    high = f.astype(BF)
    return high, (f - high.astype(F32)).astype(BF)


def face_flow(p, k, pn, kn):
    return (k * kn) / (k + kn) * (p - pn)


def wait_all(ref, sem):
    pltpu.make_async_copy(ref, ref, sem).wait()


def make_kernel(ngx, ngy, scale):
    chips_y = ngy // 2
    n = ngx * ngy

    def kernel(
        thick_h, labels_h, outlet_h, sn_h, so_h, po_h, ss_h, p_h, k_h, et_h,
        out, bal_h, top,
        thick, labels, outlet, sn, so, po, ss, et, p, k, depth, g, a0, a1, oh0, oh1, tot, half, bal,
        edge, halo, peak, peak_y, peaks_y, peaks_x, pieces, own,
        sem_small, sem_pk, sem_rest, halo_send, halo_recv, pair_send, pair_recv,
        rs_send, rs_recv, ag_send, ag_recv, pk_send, pk_recv, sem_out, main, edges,
    ):
        layers, cx, cy = sn_h.shape
        per = 2 * NP
        turns = cx // per
        early = turns * 2 // 8
        gx = lax.axis_index("gx")
        gy = lax.axis_index("gy")
        chip = gy // 2
        core = gy - chip * 2
        barrier = pltpu.get_barrier_semaphore()

        def wrap(v, m):
            return jnp.where(v >= m, v - m, v)

        chips = [wrap(chip + d, chips_y) for d in range(chips_y)]

        order = sorted(range(chips_y), key=lambda d: -min(d, chips_y - d))

        def each_chip(f):
            far = ngx * 3 // 8
            for begin, end in ((far, ngx), (1, far)):

                @pl.loop(begin, end)
                def _(i):
                    at = wrap(gx + i, ngx)
                    for d in order:
                        f(i * chips_y + d - 1, at, chips[d], d)

            for d in range(1, chips_y):
                f(d - 1, gx, chips[d], d)

        def greet(to):
            pl.semaphore_signal(barrier, inc=1, device_id=to, device_id_type=MESH)

        smalls = ((thick_h, thick), (labels_h, labels), (outlet_h, outlet))
        for i, (src, dst) in enumerate(smalls):
            pltpu.make_async_copy(src, dst, sem_small.at[i]).start()

        for i, (src, dst) in enumerate(((p_h, p), (k_h, k))):

            @pl.loop(0, layers // 16)
            def _(t, i=i, src=src, dst=dst):
                for r in range(16):
                    z = t * 16 + r
                    pltpu.make_async_copy(src.at[z], dst.at[pl.ds(0, cx), z, :], sem_pk.at[i]).start()

        rest = ((sn_h, sn), (so_h, so), (po_h, po), (ss_h, ss), (et_h, et))

        for x in range(PARTS[0]):
            for i, (src, dst) in enumerate(rest):
                pltpu.make_async_copy(src.at[:, x, :], dst.at[x], sem_rest.at[i, 0]).start()

        partner = (gx, chip * 2 + 1 - core)
        greet(partner)
        each_chip(lambda i, x, z, d: greet((x, z * 2 + core)))
        for d in range(1, chips_y):
            greet((gx, chips[d] * 2 + 1 - core))

        for part in range(1, len(PARTS)):
            rows_x = pl.ds(sum(PARTS[:part]), PARTS[part])

            @pl.loop(0, layers // 8)
            def _(t, part=part, rows_x=rows_x):
                for r in range(8):
                    z = t * 8 + r
                    for i, (src, dst) in enumerate(rest):
                        pltpu.make_async_copy(src.at[z, rows_x, :], dst.at[rows_x, z, :], sem_rest.at[i, part]).start()

        for (src, dst), i in zip(smalls, range(3)):
            pltpu.make_async_copy(src, dst, sem_small.at[i]).wait()
        for z in range(layers):
            depth[pl.ds(z, 1), :] = jnp.full((1, cy), thick[z], F32)
        p[cx] = jnp.zeros((layers, cy), F32)
        k[cx] = jnp.zeros((layers, cy), F32)
        g[...] = jnp.zeros_like(g)
        peak[...] = jnp.zeros_like(peak)
        a1[...] = jnp.zeros_like(a1)
        oh1[...] = jnp.zeros_like(oh1)
        iota = lax.broadcasted_iota(jnp.int32, (256, cy), 0).astype(F32).astype(BF)
        zero = jnp.zeros((16, cy), BF)

        def write_onehot(oh, lab, col):
            high = lab >= 256
            low = jnp.where(high, lab - 256, lab).astype(F32)
            low = jnp.broadcast_to(low, (16, cy)).astype(BF)
            lower = jnp.broadcast_to(jnp.where(high, 0.0, 1.0), (16, cy)).astype(BF)
            upper = jnp.broadcast_to(jnp.where(high, 1.0, 0.0), (16, cy)).astype(BF)
            for r in range(16):
                hit = iota[r * 16 : (r + 1) * 16] == low
                oh[r * 16 : r * 16 + 16, col] = jnp.where(hit, lower, zero)
                oh[256 + r * 16 : 272 + r * 16, col] = jnp.where(hit, upper, zero)

        lanes = lax.broadcasted_iota(jnp.int32, (layers, cy), 1)
        for i, ref in enumerate((p, k)):
            wait_all(ref.at[pl.ds(0, cx)], sem_pk.at[i])

            def take(t, carry, ref=ref):
                low, high = carry
                for r in range(8):
                    x = t * 8 + r
                    v = pltpu.roll(ref[x], x + cx, 1)
                    low = jnp.where(lanes == x + cx, v, low)
                    high = jnp.where(lanes == x + cx - 1, v, high)
                return low, high

            low, high = lax.fori_loop(0, cx // 8, take, (jnp.zeros((layers, cy), F32),) * 2)
            edge[i] = jnp.where(lanes < cx, pltpu.roll(low, cx, 1), pltpu.roll(high, 1, 1))

        def fields(x, a, oh, j):
            col = slice(j * cy, (j + 1) * cy)
            write_onehot(oh, labels[pl.ds(x, 1), :], col)
            mask = outlet[pl.ds(x, 1), :].astype(F32)
            sums = [jnp.zeros((8, cy), F32)] * 4
            top_here = peak[...]
            for zb in range(layers // ZB):
                zs = pl.ds(zb * ZB, ZB)
                d = depth[zs, :]
                pc, kc = p[x, zs, :], k[x, zs, :]
                gn = face_flow(p[x + 1, zs, :], kc, pc, k[x + 1, zs, :])
                gp = g[zs, :]
                g[zs, :] = gn
                h = face_flow(pc, kc, pltpu.roll(pc, 1, 1), pltpu.roll(kc, 1, 1))
                flux = (d + d) * (gp - gn + h - pltpu.roll(h, cy - 1, 1))
                snv, pov = sn[x, zs, :], po[x, zs, :]
                dif = snv - so[x, zs, :]
                water = d * snv * (pov + ss[x, zs, :] * pc)
                change = d * pov * dif
                uptake = d * et[x, zs, :]
                big = jnp.abs(dif)
                top_here = jnp.maximum(top_here, jnp.maximum(big[:8], big[8:]))
                for q, f in enumerate((water, change, uptake, flux)):
                    sums[q] = sums[q] + (f[:8] + f[8:])
                    high, low = split(f * mask if q == 3 else f)
                    r0 = q * layers + zb * ZB
                    a[r0 : r0 + ZB, col] = high
                    a[4 * layers + r0 : 4 * layers + r0 + ZB, col] = low
            peak[...] = top_here
            for q in range(4):
                bal[q, pl.ds(x, 1), :] = jnp.sum(sums[q], axis=0, keepdims=True)

        def product(a, oh, rows, sums, width):
            for t in range(width // 256):
                col = slice(t * 256, t * 256 + 256)
                for m in (0, 1):
                    pltpu.matmul_push_rhs(
                        oh[m * 256 : m * 256 + 256, col], staging_register=t % 2, mxu_index=m, transpose=True
                    )
                for m in (0, 1):
                    pltpu.matmul_acc_lhs(sums[m], a[:rows, col], load_staged_rhs=t % 2)
                    pltpu.matmul_acc_lhs(sums[m], a[rows : 2 * rows, col])

        def turns_of(begin, end):
            @pl.loop(begin, end)
            def _(c):
                for part, size in enumerate(PARTS):
                    begin_x = sum(PARTS[:part])
                    if begin <= begin_x // per < end:

                        @pl.when(c == begin_x // per)
                        def _(part=part, size=size, begin_x=begin_x):
                            for i, (_, dst) in enumerate(rest):
                                wait_all(dst.at[pl.ds(begin_x, size)], sem_rest.at[i, part])

                product(a1, oh1, 4 * layers, main, NP * cy)
                for j in range(NP):
                    fields(c * per + j, a0, oh0, j)
                product(a0, oh0, 4 * layers, main, NP * cy)
                for j in range(NP):
                    fields(c * per + NP + j, a1, oh1, j)

        def send(src, dst, send_sem, recv_sem, to):
            copy = pltpu.make_async_remote_copy(
                src_ref=src, dst_ref=dst, send_sem=send_sem, recv_sem=recv_sem, device_id=to, device_id_type=MESH
            )
            copy.start()
            return copy

        turns_of(0, early)
        pl.semaphore_wait(barrier, (ngx + 1) * chips_y - 1)

        x_next, x_last = wrap(gx + 1, ngx), wrap(gx + ngx - 1, ngx)
        y_next, y_last = wrap(gy + 1, ngy), wrap(gy + ngy - 1, ngy)
        halos = []
        for i, ref in enumerate((p, k)):
            for slot, src, to in (
                (i, ref.at[cx - 1], (x_next, gy)),
                (2 + i, ref.at[0], (x_last, gy)),
                (4 + i, edge.at[i], (gx, y_next)),
                (6 + i, edge.at[i], (gx, y_last)),
            ):
                halos.append(send(src, halo.at[slot], halo_send.at[slot], halo_recv.at[slot], to))

        turns_of(early, turns)

        peak[...] = jnp.broadcast_to(jnp.max(peak[...], axis=0, keepdims=True), (8, cy))

        @pl.loop(1, ngx)
        def _(d):
            send(peak.at[:1, :], peaks_x.at[d - 1], pk_send.at[0], pk_recv.at[0], (wrap(gx + d, ngx), gy))

        for h in halos:
            h.wait()
        product(a1, oh1, 4 * layers, main, NP * cy)
        left = lanes < cx
        ly = jnp.concatenate([labels[...]] * 2, axis=0).astype(F32).T
        oy = jnp.concatenate([outlet[...]] * 2, axis=0).astype(F32).T
        first = lax.broadcasted_iota(jnp.int32, (1, cy), 1) < cx
        lab_y = jnp.where(first, ly[:1], ly[cy - 1 :]).astype(jnp.int32)
        out_y = jnp.where(first, oy[:1], oy[cy - 1 :])
        d2 = depth[...] + depth[...]
        py = jnp.where(left, pltpu.roll(halo[4], cx, 1), pltpu.roll(halo[6], cx, 1))
        ky = jnp.where(left, pltpu.roll(halo[5], cx, 1), pltpu.roll(halo[7], cx, 1))
        inside = jnp.where(left, jnp.where(gy > 0, 1.0, 0.0), jnp.where(gy < ngy - 1, 1.0, 0.0))
        borders = (
            (p[0], k[0], halo[0], halo[1] * jnp.where(gx > 0, 1.0, 0.0), labels[:1, :], outlet[:1, :].astype(F32)),
            (
                p[cx - 1], k[cx - 1], halo[2], halo[3] * jnp.where(gx < ngx - 1, 1.0, 0.0),
                labels[cx - 1 :, :], outlet[cx - 1 :, :].astype(F32),
            ),
            (edge[0], edge[1], py, ky * inside, lab_y, out_y),
        )
        for i, (pc, kc, pn, kn, lab, mask) in enumerate(borders):
            f = face_flow(pc, kc, pn, kn)
            if i == 2:
                f = f - face_flow(pc, kc, pltpu.roll(pc, cx, 1), pltpu.roll(kc, cx, 1))
            f = d2 * f
            col = slice(i * cy, (i + 1) * cy)
            write_onehot(oh0, lab, col)
            high, low = split(f * mask)
            a0[:layers, col] = high
            a0[layers : 2 * layers, col] = low
            f = jnp.sum(f, axis=0, keepdims=True)
            if i < 2:
                x = i * (cx - 1)
                bal[3, x : x + 1, :] += f
            else:
                ft = jnp.broadcast_to(f, (8, cy)).T
                at = lax.broadcasted_iota(jnp.int32, (cx, cy), 1)
                low_side = jnp.where(at == 0, jnp.broadcast_to(ft[:cx, :1], (cx, cy)), 0.0)
                high_side = jnp.where(at == cy - 1, jnp.broadcast_to(ft[cx:, :1], (cx, cy)), 0.0)
                bal[3] += low_side + high_side
        a0[: 2 * layers, 3 * cy : 4 * cy] = jnp.zeros((2 * layers, cy), BF)
        product(a0, oh0, layers, edges, 4 * cy)
        for m in (0, 1):
            col = slice(m * 256, m * 256 + 256)
            r = pltpu.matmul_pop(main[m])
            tot[: 3 * layers, col] = r[: 3 * layers]
            tot[3 * layers :, col] = r[3 * layers :] + pltpu.matmul_pop(edges[m])

        rows = 2 * layers
        mine, theirs = (pl.multiple_of(v * rows, rows) for v in (core, 1 - core))
        pair = send(tot.at[pl.ds(theirs, rows), :], half, pair_send.at[0], pair_recv.at[0], partner)
        bal_copy = pltpu.make_async_copy(bal, bal_h, sem_out.at[0])
        bal_copy.start()

        pair.wait()
        tot[pl.ds(mine, rows), :] += half[...]

        def tile(ref, x, z):
            return ref.at[
                pl.ds(pl.multiple_of(core * rows + x * 8, 8), 8), pl.ds(pl.multiple_of(z * 128, 128), 128)
            ]

        each_chip(lambda i, x, z, d: send(tile(tot, x, z), pieces.at[i], rs_send, rs_recv, (x, z * 2 + core)))

        wait_all(pieces, rs_recv)
        terms = [tile(tot, gx, chip)[...]] + [pieces[d] for d in range(n // 2 - 1)]
        while len(terms) > 1:
            terms = [a + b for a, b in zip(terms[::2], terms[1::2])] + terms[len(terms) // 2 * 2 :]
        own[...] = terms[0] * scale

        here = tile(out, gx, chip)
        each_chip(lambda i, x, z, d: send(own, here, ag_send, ag_recv.at[d], (x, z * 2 + core)))
        own_copy = pltpu.make_async_copy(own, here, sem_out.at[1])
        own_copy.start()
        wait_all(peaks_x, pk_recv.at[0])
        wait_all(peaks_x, pk_send.at[0])
        best = peak[:1, :]
        for d in range(ngx - 1):
            best = jnp.maximum(best, peaks_x[d])
        peak_y[...] = best
        for d in range(1, ngy):
            send(peak_y, peaks_y.at[d - 1], pk_send.at[1], pk_recv.at[1], (gx, wrap(gy + d, ngy)))
        bal_copy.wait()
        wait_all(pieces, rs_send)
        own_copy.wait()
        passed = []
        for d in reversed(order):
            wait_all(pieces.at[pl.ds(0, ngx - (d == 0))], ag_recv.at[d])
            source = wrap(chip + chips_y - d, chips_y)
            block = out.at[pl.ds(mine, rows), pl.ds(pl.multiple_of(source * 128, 128), 128)]
            passed.append(send(block, block, pair_send.at[1 + d], pair_recv.at[1 + d], partner))
        wait_all(pieces, ag_send)
        wait_all(peaks_y, pk_recv.at[1])
        wait_all(peaks_y, pk_send.at[1])
        for d in range(ngy - 1):
            best = jnp.maximum(best, peaks_y[d])
        top[0] = jnp.max(best)
        for copy in passed:
            copy.wait()

    def with_sums(*refs):
        layers = refs[3].shape[0]

        def body(main_0, main_1, edge_0, edge_1):
            for r in (main_0, main_1, edge_0, edge_1):
                pltpu.matmul_pop(r)
            kernel(*refs, (main_0, main_1), (edge_0, edge_1))

        pl.run_scoped(
            body,
            pltpu.ACC(0)((4 * layers, 256), F32), pltpu.ACC(1)((4 * layers, 256), F32),
            pltpu.ACC(0)((layers, 256), F32), pltpu.ACC(1)((layers, 256), F32),
        )

    return with_sums


def solution(mesh):
    ngx, ngy = mesh.shape["gx"], mesh.shape["gy"]
    n = ngx * ngy

    def on_device(sat_new, sat_old, porosity, spec_storage, pressure, conduct, et_rate, thickness, labels, outlet):
        layers, cx, cy = sat_new.shape
        scale = layers * SUB / (ngx * cx * ngy * cy)
        field = pltpu.VMEM((cx, layers, cy), F32)
        longer = pltpu.VMEM((cx + 1, layers, cy), F32)
        sheet = pltpu.VMEM((layers, cy), F32)
        dma = pltpu.SemaphoreType.DMA
        anywhere = pl.BlockSpec(memory_space=pl.ANY)
        out, bal, top = pl.pallas_call(
            make_kernel(ngx, ngy, scale),
            out_shape=(
                jax.ShapeDtypeStruct((4 * layers, SUB), F32),
                jax.ShapeDtypeStruct((4, cx, cy), F32),
                jax.ShapeDtypeStruct((1,), F32),
            ),
            in_specs=[pl.BlockSpec(memory_space=pltpu.HBM)] * 10,
            out_specs=(anywhere, anywhere, pl.BlockSpec(memory_space=pltpu.SMEM)),
            scratch_shapes=[
                pltpu.SMEM((layers,), F32),
                pltpu.VMEM((cx, cy), jnp.int32),
                pltpu.VMEM((cx, cy), jnp.int32),
                field, field, field, field, field, longer, longer,
                sheet,
                sheet,
                pltpu.VMEM((8 * layers, NP * cy), BF),
                pltpu.VMEM((8 * layers, NP * cy), BF),
                pltpu.VMEM((SUB, NP * cy), BF),
                pltpu.VMEM((SUB, NP * cy), BF),
                pltpu.VMEM((4 * layers, SUB), F32),
                pltpu.VMEM((2 * layers, SUB), F32),
                pltpu.VMEM((4, cx, cy), F32),
                pltpu.VMEM((2, layers, cy), F32),
                pltpu.VMEM((8, layers, cy), F32),
                pltpu.VMEM((8, cy), F32),
                pltpu.VMEM((1, cy), F32),
                pltpu.VMEM((ngy - 1, 1, cy), F32),
                pltpu.VMEM((ngx - 1, 1, cy), F32),
                pltpu.VMEM((n // 2 - 1, 8, 128), F32),
                pltpu.VMEM((8, 128), F32),
                dma((3,)), dma((2,)), dma((5, len(PARTS))), dma((8,)), dma((8,)), dma((1 + ngy // 2,)), dma((1 + ngy // 2,)),
                dma, dma, dma, dma((ngy // 2,)), dma((2,)), dma((2,)), dma((2,)),
            ],
            compiler_params=pltpu.CompilerParams(
                collective_id=0, has_side_effects=True, vmem_limit_bytes=48 << 20
            ),
            name="balance",
        )(*(
            pltpu.with_memory_space_constraint(v, pltpu.HBM)
            for v in (thickness, labels, outlet, sat_new, sat_old, porosity, spec_storage, pressure, conduct, et_rate)
        ))
        return out.reshape(4, layers, SUB), bal, top.reshape(())

    cells = P(None, "gx", "gy")
    return jax.shard_map(
        on_device,
        mesh=mesh,
        in_specs=(cells,) * 7 + (P(), P("gx", "gy"), P("gx", "gy")),
        out_specs=(P(), cells, P()),
        check_vma=False,
    )
```

```python
import jax
import jax.numpy as jnp
from jax import lax
from jax.experimental import pallas as pl
from jax.experimental.pallas import tpu as pltpu
from jax.sharding import PartitionSpec as P

SUB = 512
NP = 4
ZB = 16
PARTS = (8, 24, 32)
MESH = pl.DeviceIdType.MESH
BF = jnp.bfloat16
F32 = jnp.float32


def split(f):
    high = f.astype(BF)
    return high, (f - high.astype(F32)).astype(BF)


def face_flow(p, k, pn, kn):
    return (k * kn) / (k + kn) * (p - pn)


def wait_all(ref, sem):
    pltpu.make_async_copy(ref, ref, sem).wait()


def make_kernel(ngx, ngy, scale):
    chips_y = ngy // 2
    n = ngx * ngy

    def kernel(
        thick_h, labels_h, outlet_h, sn_h, so_h, po_h, ss_h, p_h, k_h, et_h,
        out, bal_h, top,
        thick, labels, outlet, sn, so, po, ss, et, p, k, depth, g, a0, a1, oh0, oh1, tot, half, bal,
        edge, halo, peak, peak_y, peaks_y, peaks_x, pieces, own,
        sem_small, sem_pk, sem_rest, halo_send, halo_recv, pair_send, pair_recv,
        rs_send, rs_recv, ag_send, ag_recv, pk_send, pk_recv, sem_out, main, edges,
    ):
        layers, cx, cy = sn_h.shape
        per = 2 * NP
        turns = cx // per
        early = turns * 2 // 8
        gx = lax.axis_index("gx")
        gy = lax.axis_index("gy")
        chip = gy // 2
        core = gy - chip * 2
        barrier = pltpu.get_barrier_semaphore()

        def wrap(v, m):
            return jnp.where(v >= m, v - m, v)

        chips = [wrap(chip + d, chips_y) for d in range(chips_y)]

        order = sorted(range(chips_y), key=lambda d: -min(d, chips_y - d))

        def each_chip(f):
            far = ngx * 3 // 8
            for begin, end in ((far, ngx), (1, far)):

                @pl.loop(begin, end)
                def _(i):
                    at = wrap(gx + i, ngx)
                    for d in order:
                        f(i * chips_y + d - 1, at, chips[d], d)

            for d in range(1, chips_y):
                f(d - 1, gx, chips[d], d)

        def greet(to):
            pl.semaphore_signal(barrier, inc=1, device_id=to, device_id_type=MESH)

        smalls = ((thick_h, thick), (labels_h, labels), (outlet_h, outlet))
        for i, (src, dst) in enumerate(smalls):
            pltpu.make_async_copy(src, dst, sem_small.at[i]).start()

        for i, (src, dst) in enumerate(((p_h, p), (k_h, k))):

            @pl.loop(0, layers // 16)
            def _(t, i=i, src=src, dst=dst):
                for r in range(16):
                    z = t * 16 + r
                    pltpu.make_async_copy(src.at[z], dst.at[pl.ds(0, cx), z, :], sem_pk.at[i]).start()

        rest = ((sn_h, sn), (so_h, so), (po_h, po), (ss_h, ss), (et_h, et))

        for x in range(PARTS[0]):
            for i, (src, dst) in enumerate(rest):
                pltpu.make_async_copy(src.at[:, x, :], dst.at[x], sem_rest.at[i, 0]).start()

        partner = (gx, chip * 2 + 1 - core)
        greet(partner)
        each_chip(lambda i, x, z, d: greet((x, z * 2 + core)))
        for d in range(1, chips_y):
            greet((gx, chips[d] * 2 + 1 - core))

        for part in range(1, len(PARTS)):
            rows_x = pl.ds(sum(PARTS[:part]), PARTS[part])

            @pl.loop(0, layers // 8)
            def _(t, part=part, rows_x=rows_x):
                for r in range(8):
                    z = t * 8 + r
                    for i, (src, dst) in enumerate(rest):
                        pltpu.make_async_copy(src.at[z, rows_x, :], dst.at[rows_x, z, :], sem_rest.at[i, part]).start()

        for (src, dst), i in zip(smalls, range(3)):
            pltpu.make_async_copy(src, dst, sem_small.at[i]).wait()
        for z in range(layers):
            depth[pl.ds(z, 1), :] = jnp.full((1, cy), thick[z], F32)
        p[cx] = jnp.zeros((layers, cy), F32)
        k[cx] = jnp.zeros((layers, cy), F32)
        g[...] = jnp.zeros_like(g)
        peak[...] = jnp.zeros_like(peak)
        a1[...] = jnp.zeros_like(a1)
        oh1[...] = jnp.zeros_like(oh1)
        iota = lax.broadcasted_iota(jnp.int32, (256, cy), 0).astype(F32).astype(BF)
        zero = jnp.zeros((16, cy), BF)

        def write_onehot(oh, lab, col):
            high = lab >= 256
            low = jnp.where(high, lab - 256, lab).astype(F32)
            low = jnp.broadcast_to(low, (16, cy)).astype(BF)
            lower = jnp.broadcast_to(jnp.where(high, 0.0, 1.0), (16, cy)).astype(BF)
            upper = jnp.broadcast_to(jnp.where(high, 1.0, 0.0), (16, cy)).astype(BF)
            for r in range(16):
                hit = iota[r * 16 : (r + 1) * 16] == low
                oh[r * 16 : r * 16 + 16, col] = jnp.where(hit, lower, zero)
                oh[256 + r * 16 : 272 + r * 16, col] = jnp.where(hit, upper, zero)

        lanes = lax.broadcasted_iota(jnp.int32, (layers, cy), 1)
        for i, ref in enumerate((p, k)):
            wait_all(ref.at[pl.ds(0, cx)], sem_pk.at[i])

            def take(t, carry, ref=ref):
                low, high = carry
                for r in range(8):
                    x = t * 8 + r
                    v = pltpu.roll(ref[x], x + cx, 1)
                    low = jnp.where(lanes == x + cx, v, low)
                    high = jnp.where(lanes == x + cx - 1, v, high)
                return low, high

            low, high = lax.fori_loop(0, cx // 8, take, (jnp.zeros((layers, cy), F32),) * 2)
            edge[i] = jnp.where(lanes < cx, pltpu.roll(low, cx, 1), pltpu.roll(high, 1, 1))

        def fields(x, a, oh, j):
            col = slice(j * cy, (j + 1) * cy)
            write_onehot(oh, labels[pl.ds(x, 1), :], col)
            mask = outlet[pl.ds(x, 1), :].astype(F32)
            sums = [jnp.zeros((8, cy), F32)] * 4
            top_here = peak[...]
            for zb in range(layers // ZB):
                zs = pl.ds(zb * ZB, ZB)
                d = depth[zs, :]
                pc, kc = p[x, zs, :], k[x, zs, :]
                gn = face_flow(p[x + 1, zs, :], kc, pc, k[x + 1, zs, :])
                gp = g[zs, :]
                g[zs, :] = gn
                h = face_flow(pc, kc, pltpu.roll(pc, 1, 1), pltpu.roll(kc, 1, 1))
                flux = (d + d) * (gp - gn + h - pltpu.roll(h, cy - 1, 1))
                snv, pov = sn[x, zs, :], po[x, zs, :]
                dif = snv - so[x, zs, :]
                water = d * snv * (pov + ss[x, zs, :] * pc)
                change = d * pov * dif
                uptake = d * et[x, zs, :]
                big = jnp.abs(dif)
                top_here = jnp.maximum(top_here, jnp.maximum(big[:8], big[8:]))
                for q, f in enumerate((water, change, uptake, flux)):
                    sums[q] = sums[q] + (f[:8] + f[8:])
                    high, low = split(f * mask if q == 3 else f)
                    r0 = q * layers + zb * ZB
                    a[r0 : r0 + ZB, col] = high
                    a[4 * layers + r0 : 4 * layers + r0 + ZB, col] = low
            peak[...] = top_here
            for q in range(4):
                bal[q, pl.ds(x, 1), :] = jnp.sum(sums[q], axis=0, keepdims=True)

        def product(a, oh, rows, sums, width):
            for t in range(width // 256):
                col = slice(t * 256, t * 256 + 256)
                for m in (0, 1):
                    pltpu.matmul_push_rhs(
                        oh[m * 256 : m * 256 + 256, col], staging_register=t % 2, mxu_index=m, transpose=True
                    )
                for m in (0, 1):
                    pltpu.matmul_acc_lhs(sums[m], a[:rows, col], load_staged_rhs=t % 2)
                    pltpu.matmul_acc_lhs(sums[m], a[rows : 2 * rows, col])

        def turns_of(begin, end):
            @pl.loop(begin, end)
            def _(c):
                for part, size in enumerate(PARTS):
                    begin_x = sum(PARTS[:part])
                    if begin <= begin_x // per < end:

                        @pl.when(c == begin_x // per)
                        def _(part=part, size=size, begin_x=begin_x):
                            for i, (_, dst) in enumerate(rest):
                                wait_all(dst.at[pl.ds(begin_x, size)], sem_rest.at[i, part])

                product(a1, oh1, 4 * layers, main, NP * cy)
                for j in range(NP):
                    fields(c * per + j, a0, oh0, j)
                product(a0, oh0, 4 * layers, main, NP * cy)
                for j in range(NP):
                    fields(c * per + NP + j, a1, oh1, j)

        def send(src, dst, send_sem, recv_sem, to):
            copy = pltpu.make_async_remote_copy(
                src_ref=src, dst_ref=dst, send_sem=send_sem, recv_sem=recv_sem, device_id=to, device_id_type=MESH
            )
            copy.start()
            return copy

        turns_of(0, early)
        pl.semaphore_wait(barrier, (ngx + 1) * chips_y - 1)

        x_next, x_last = wrap(gx + 1, ngx), wrap(gx + ngx - 1, ngx)
        y_next, y_last = wrap(gy + 1, ngy), wrap(gy + ngy - 1, ngy)
        halos = []
        for i, ref in enumerate((p, k)):
            for slot, src, to in (
                (i, ref.at[cx - 1], (x_next, gy)),
                (2 + i, ref.at[0], (x_last, gy)),
                (4 + i, edge.at[i], (gx, y_next)),
                (6 + i, edge.at[i], (gx, y_last)),
            ):
                halos.append(send(src, halo.at[slot], halo_send.at[slot], halo_recv.at[slot], to))

        turns_of(early, turns)

        for h in halos:
            h.wait()
        product(a1, oh1, 4 * layers, main, NP * cy)
        left = lanes < cx
        ly = jnp.concatenate([labels[...]] * 2, axis=0).astype(F32).T
        oy = jnp.concatenate([outlet[...]] * 2, axis=0).astype(F32).T
        first = lax.broadcasted_iota(jnp.int32, (1, cy), 1) < cx
        lab_y = jnp.where(first, ly[:1], ly[cy - 1 :]).astype(jnp.int32)
        out_y = jnp.where(first, oy[:1], oy[cy - 1 :])
        d2 = depth[...] + depth[...]
        py = jnp.where(left, pltpu.roll(halo[4], cx, 1), pltpu.roll(halo[6], cx, 1))
        ky = jnp.where(left, pltpu.roll(halo[5], cx, 1), pltpu.roll(halo[7], cx, 1))
        inside = jnp.where(left, jnp.where(gy > 0, 1.0, 0.0), jnp.where(gy < ngy - 1, 1.0, 0.0))
        borders = (
            (p[0], k[0], halo[0], halo[1] * jnp.where(gx > 0, 1.0, 0.0), labels[:1, :], outlet[:1, :].astype(F32)),
            (
                p[cx - 1], k[cx - 1], halo[2], halo[3] * jnp.where(gx < ngx - 1, 1.0, 0.0),
                labels[cx - 1 :, :], outlet[cx - 1 :, :].astype(F32),
            ),
            (edge[0], edge[1], py, ky * inside, lab_y, out_y),
        )
        for i, (pc, kc, pn, kn, lab, mask) in enumerate(borders):
            f = face_flow(pc, kc, pn, kn)
            if i == 2:
                f = f - face_flow(pc, kc, pltpu.roll(pc, cx, 1), pltpu.roll(kc, cx, 1))
            f = d2 * f
            col = slice(i * cy, (i + 1) * cy)
            write_onehot(oh0, lab, col)
            high, low = split(f * mask)
            a0[:layers, col] = high
            a0[layers : 2 * layers, col] = low
            f = jnp.sum(f, axis=0, keepdims=True)
            if i < 2:
                x = i * (cx - 1)
                bal[3, x : x + 1, :] += f
            else:
                ft = jnp.broadcast_to(f, (8, cy)).T
                at = lax.broadcasted_iota(jnp.int32, (cx, cy), 1)
                low_side = jnp.where(at == 0, jnp.broadcast_to(ft[:cx, :1], (cx, cy)), 0.0)
                high_side = jnp.where(at == cy - 1, jnp.broadcast_to(ft[cx:, :1], (cx, cy)), 0.0)
                bal[3] += low_side + high_side
        a0[: 2 * layers, 3 * cy : 4 * cy] = jnp.zeros((2 * layers, cy), BF)
        product(a0, oh0, layers, edges, 4 * cy)
        for m in (0, 1):
            col = slice(m * 256, m * 256 + 256)
            r = pltpu.matmul_pop(main[m])
            tot[: 3 * layers, col] = r[: 3 * layers]
            tot[3 * layers :, col] = r[3 * layers :] + pltpu.matmul_pop(edges[m])

        rows = 2 * layers
        mine, theirs = (pl.multiple_of(v * rows, rows) for v in (core, 1 - core))
        pair = send(tot.at[pl.ds(theirs, rows), :], half, pair_send.at[0], pair_recv.at[0], partner)
        bal_copy = pltpu.make_async_copy(bal, bal_h, sem_out.at[0])
        bal_copy.start()

        peak[...] = jnp.broadcast_to(jnp.max(peak[...], axis=0, keepdims=True), (8, cy))

        @pl.loop(1, ngx)
        def _(d):
            send(peak.at[:1, :], peaks_x.at[d - 1], pk_send.at[0], pk_recv.at[0], (wrap(gx + d, ngx), gy))


        pair.wait()
        tot[pl.ds(mine, rows), :] += half[...]

        def tile(ref, x, z):
            return ref.at[
                pl.ds(pl.multiple_of(core * rows + x * 8, 8), 8), pl.ds(pl.multiple_of(z * 128, 128), 128)
            ]

        each_chip(lambda i, x, z, d: send(tile(tot, x, z), pieces.at[i], rs_send, rs_recv, (x, z * 2 + core)))

        wait_all(pieces, rs_recv)
        terms = [tile(tot, gx, chip)[...]] + [pieces[d] for d in range(n // 2 - 1)]
        while len(terms) > 1:
            terms = [a + b for a, b in zip(terms[::2], terms[1::2])] + terms[len(terms) // 2 * 2 :]
        own[...] = terms[0] * scale

        here = tile(out, gx, chip)
        each_chip(lambda i, x, z, d: send(own, here, ag_send, ag_recv.at[d], (x, z * 2 + core)))
        own_copy = pltpu.make_async_copy(own, here, sem_out.at[1])
        own_copy.start()
        wait_all(peaks_x, pk_recv.at[0])
        wait_all(peaks_x, pk_send.at[0])
        best = peak[:1, :]
        for d in range(ngx - 1):
            best = jnp.maximum(best, peaks_x[d])
        peak_y[...] = best
        for d in range(1, ngy):
            send(peak_y, peaks_y.at[d - 1], pk_send.at[1], pk_recv.at[1], (gx, wrap(gy + d, ngy)))
        bal_copy.wait()
        wait_all(pieces, rs_send)
        own_copy.wait()
        passed = []
        for d in reversed(order):
            wait_all(pieces.at[pl.ds(0, ngx - (d == 0))], ag_recv.at[d])
            source = wrap(chip + chips_y - d, chips_y)
            block = out.at[pl.ds(mine, rows), pl.ds(pl.multiple_of(source * 128, 128), 128)]
            passed.append(send(block, block, pair_send.at[1 + d], pair_recv.at[1 + d], partner))
        wait_all(pieces, ag_send)
        wait_all(peaks_y, pk_recv.at[1])
        wait_all(peaks_y, pk_send.at[1])
        for d in range(ngy - 1):
            best = jnp.maximum(best, peaks_y[d])
        top[0] = jnp.max(best)
        for copy in passed:
            copy.wait()

    def with_sums(*refs):
        layers = refs[3].shape[0]

        def body(main_0, main_1, edge_0, edge_1):
            for r in (main_0, main_1, edge_0, edge_1):
                pltpu.matmul_pop(r)
            kernel(*refs, (main_0, main_1), (edge_0, edge_1))

        pl.run_scoped(
            body,
            pltpu.ACC(0)((4 * layers, 256), F32), pltpu.ACC(1)((4 * layers, 256), F32),
            pltpu.ACC(0)((layers, 256), F32), pltpu.ACC(1)((layers, 256), F32),
        )

    return with_sums


def solution(mesh):
    ngx, ngy = mesh.shape["gx"], mesh.shape["gy"]
    n = ngx * ngy

    def on_device(sat_new, sat_old, porosity, spec_storage, pressure, conduct, et_rate, thickness, labels, outlet):
        layers, cx, cy = sat_new.shape
        scale = layers * SUB / (ngx * cx * ngy * cy)
        field = pltpu.VMEM((cx, layers, cy), F32)
        longer = pltpu.VMEM((cx + 1, layers, cy), F32)
        sheet = pltpu.VMEM((layers, cy), F32)
        dma = pltpu.SemaphoreType.DMA
        anywhere = pl.BlockSpec(memory_space=pl.ANY)
        out, bal, top = pl.pallas_call(
            make_kernel(ngx, ngy, scale),
            out_shape=(
                jax.ShapeDtypeStruct((4 * layers, SUB), F32),
                jax.ShapeDtypeStruct((4, cx, cy), F32),
                jax.ShapeDtypeStruct((1,), F32),
            ),
            in_specs=[pl.BlockSpec(memory_space=pltpu.HBM)] * 10,
            out_specs=(anywhere, anywhere, pl.BlockSpec(memory_space=pltpu.SMEM)),
            scratch_shapes=[
                pltpu.SMEM((layers,), F32),
                pltpu.VMEM((cx, cy), jnp.int32),
                pltpu.VMEM((cx, cy), jnp.int32),
                field, field, field, field, field, longer, longer,
                sheet,
                sheet,
                pltpu.VMEM((8 * layers, NP * cy), BF),
                pltpu.VMEM((8 * layers, NP * cy), BF),
                pltpu.VMEM((SUB, NP * cy), BF),
                pltpu.VMEM((SUB, NP * cy), BF),
                pltpu.VMEM((4 * layers, SUB), F32),
                pltpu.VMEM((2 * layers, SUB), F32),
                pltpu.VMEM((4, cx, cy), F32),
                pltpu.VMEM((2, layers, cy), F32),
                pltpu.VMEM((8, layers, cy), F32),
                pltpu.VMEM((8, cy), F32),
                pltpu.VMEM((1, cy), F32),
                pltpu.VMEM((ngy - 1, 1, cy), F32),
                pltpu.VMEM((ngx - 1, 1, cy), F32),
                pltpu.VMEM((n // 2 - 1, 8, 128), F32),
                pltpu.VMEM((8, 128), F32),
                dma((3,)), dma((2,)), dma((5, len(PARTS))), dma((8,)), dma((8,)), dma((1 + ngy // 2,)), dma((1 + ngy // 2,)),
                dma, dma, dma, dma((ngy // 2,)), dma((2,)), dma((2,)), dma((2,)),
            ],
            compiler_params=pltpu.CompilerParams(
                collective_id=0, has_side_effects=True, vmem_limit_bytes=48 << 20
            ),
            name="balance",
        )(*(
            pltpu.with_memory_space_constraint(v, pltpu.HBM)
            for v in (thickness, labels, outlet, sat_new, sat_old, porosity, spec_storage, pressure, conduct, et_rate)
        ))
        return out.reshape(4, layers, SUB), bal, top.reshape(())

    cells = P(None, "gx", "gy")
    return jax.shard_map(
        on_device,
        mesh=mesh,
        in_specs=(cells,) * 7 + (P(), P("gx", "gy"), P("gx", "gy")),
        out_specs=(P(), cells, P()),
        check_vma=False,
    )
```
